8 devices in a mesh: dp: 1 (over z), etp: 2 (over y), ep: 4 (over x, core).
Axes of the slice: x: 2, y: 2, z: 1, core: 2. Of those that a mesh axis runs over, the one named last changes fastest.
Arguments:
- u_rows: bfloat16 [512, 1536], P(('dp', 'ep', 'etp'))
- dy_rows: bfloat16 [512, 1536], P(('dp', 'ep', 'etp'))
- topk_ids: int32 [512, 8], P(('dp', 'ep', 'etp'))
- w_router: bfloat16 [1536, 40], replicated
- w_gate: bfloat16 [40, 1536, 512], P('ep', None, 'etp')
- w_up: bfloat16 [40, 1536, 512], P('ep', None, 'etp')
- w_down: bfloat16 [40, 512, 1536], P('ep', 'etp')
Outputs:
- output 1: bfloat16 [512, 1536], P(('dp', 'ep', 'etp'))
- output 2: bfloat16 [512, 1536], P(('dp', 'ep', 'etp'))
- output 3: float32 [40, 1536, 512], P(('dp', 'ep'), None, 'etp')
- output 4: float32 [40, 1536, 512], P(('dp', 'ep'), None, 'etp')
- output 5: float32 [40, 512, 1536], P(('dp', 'ep'), 'etp')
- output 6: float32 [1536, 40], P('dp')
All inputs are finite; a program needn't handle non-finite values.
Results may differ from the reference program's by a relative error of at most 0.010856.
Values are sent between devices in bfloat16 or wider.
A program may use at most 1 GiB of HBM per device.

```python
import jax
import jax.numpy as jnp
from jax import lax

TOK_DEV = 64
SHARDS = 8
D_MODEL = 1536
EXPERTS = 40
TOP_K = 8
FFN = 512
TOKENS = TOK_DEV * SHARDS
CAP = min(TOK_DEV, (4 * TOK_DEV * TOP_K + EXPERTS - 1) // EXPERTS)
EXP_ROWS = SHARDS * CAP


def shard_ids(shard_key):
    key_perm, key_rank = jax.random.split(shard_key)
    expert_perm = jax.random.permutation(key_perm, EXPERTS)
    tok_rank = jax.random.permutation(key_rank, TOK_DEV)
    hot_expert = expert_perm[EXPERTS - 1]
    slot_col = jnp.arange(TOP_K)[None, :]
    has_hot = (tok_rank < CAP)[:, None]
    base_pos = tok_rank * TOP_K - jnp.minimum(tok_rank, CAP)
    cyc_pos = (base_pos[:, None] + slot_col - has_hot.astype(jnp.int32)) % (EXPERTS - 1)
    chosen = jnp.where(has_hot & (slot_col == 0), hot_expert, expert_perm[cyc_pos])
    return chosen.astype(jnp.int32)


def setup_inputs(seed: int = 0, part: int = 0) -> dict:
    part_key = jax.random.fold_in(jax.random.key(seed), part)
    key_tok, key_cot, key_route = jax.random.split(part_key, 3)
    key_router, key_gate, key_up, key_down = jax.random.split(jax.random.key(seed + 1), 4)
    topk_ids = jax.vmap(shard_ids)(jax.random.split(key_route, SHARDS)).reshape(TOKENS, TOP_K)
    u_rows = jax.random.normal(key_tok, (TOKENS, D_MODEL), jnp.float32).astype(jnp.bfloat16)
    dy_rows = jax.random.normal(key_cot, (TOKENS, D_MODEL), jnp.float32).astype(jnp.bfloat16)
    w_router = (jax.random.normal(key_router, (D_MODEL, EXPERTS), jnp.float32) * D_MODEL ** -0.5).astype(jnp.bfloat16)
    w_gate = (jax.random.normal(key_gate, (EXPERTS, D_MODEL, FFN), jnp.float32) * D_MODEL ** -0.5).astype(jnp.bfloat16)
    w_up = (jax.random.normal(key_up, (EXPERTS, D_MODEL, FFN), jnp.float32) * D_MODEL ** -0.5).astype(jnp.bfloat16)
    down_scale = 4.0 * EXPERTS / TOP_K * FFN ** -0.5
    w_down = (jax.random.normal(key_down, (EXPERTS, FFN, D_MODEL), jnp.float32) * down_scale).astype(jnp.bfloat16)
    return {"u_rows": u_rows, "dy_rows": dy_rows, "topk_ids": topk_ids, "w_router": w_router, "w_gate": w_gate, "w_up": w_up, "w_down": w_down}


def one_expert(u_wide, tok_rows, gate_rows, gate_e, up_e, down_e):
    x_rows = u_wide[tok_rows]
    h_gate = jnp.dot(x_rows, gate_e, preferred_element_type=jnp.float32).astype(jnp.bfloat16).astype(jnp.float32)
    h_up = jnp.dot(x_rows, up_e, preferred_element_type=jnp.float32).astype(jnp.bfloat16).astype(jnp.float32)
    act_rows = (jax.nn.silu(h_gate) * h_up).astype(jnp.bfloat16).astype(jnp.float32)
    out_rows = jnp.dot(act_rows, down_e, preferred_element_type=jnp.float32).astype(jnp.bfloat16).astype(jnp.float32)
    return gate_rows[:, None] * out_rows


def moe_forward(u_wide, topk_ids, router_wide, gate_wide, up_wide, down_wide):
    logits = jnp.dot(u_wide, router_wide, preferred_element_type=jnp.float32)
    router_prob = jax.nn.softmax(logits, axis=-1)
    gate_vals = jnp.take_along_axis(router_prob, topk_ids, axis=1).reshape(-1)
    flat_ids = topk_ids.reshape(-1)
    pair_order = jnp.argsort(flat_ids, stable=True)
    counts = jnp.bincount(flat_ids, length=EXPERTS)
    starts = jnp.cumsum(counts) - counts
    row_pos = jnp.arange(EXP_ROWS)
    is_valid = row_pos[None, :] < counts[:, None]
    pair_idx = pair_order[jnp.minimum(starts[:, None] + row_pos[None, :], TOKENS * TOP_K - 1)]
    tok_idx = pair_idx // TOP_K
    row_gate = jnp.where(is_valid, gate_vals[pair_idx], 0.0)
    expert_fn = jax.checkpoint(one_expert)

    def expert_step(moe_sum, per_expert):
        tok_rows, gate_rows, gate_e, up_e, down_e = per_expert
        contrib = expert_fn(u_wide, tok_rows, gate_rows, gate_e, up_e, down_e)
        return moe_sum.at[tok_rows].add(contrib), None

    moe_sum, unused = lax.scan(expert_step, jnp.zeros((TOKENS, D_MODEL), jnp.float32), (tok_idx, row_gate, gate_wide, up_wide, down_wide))
    return (u_wide + moe_sum).astype(jnp.bfloat16)


def reference(u_rows, dy_rows, topk_ids, w_router, w_gate, w_up, w_down):
    def forward(u_wide, router_wide, gate_wide, up_wide, down_wide):
        return moe_forward(u_wide, topk_ids, router_wide, gate_wide, up_wide, down_wide)

    y_rows, pull_back = jax.vjp(forward, u_rows.astype(jnp.float32), w_router.astype(jnp.float32), w_gate.astype(jnp.float32), w_up.astype(jnp.float32), w_down.astype(jnp.float32))
    du_wide, dw_router, dw_gate, dw_up, dw_down = pull_back(dy_rows)
    return y_rows, du_wide.astype(jnp.bfloat16), dw_gate, dw_up, dw_down, dw_router
```

```python
import functools

import jax
import jax.numpy as jnp
from jax import lax
from jax.experimental import pallas as pl
from jax.experimental.pallas import tpu as pltpu
from jax.sharding import PartitionSpec as P

MESH = pl.DeviceIdType.MESH
F32 = jnp.float32
BF16 = jnp.bfloat16
LANES = 128
GROUP = 16
OWN, DIAG, XN, YN = 0, 1, 2, 3


def dot(a, b):
    return jnp.dot(a, b, preferred_element_type=F32)


def dot_t(a, b):
    return lax.dot_general(a, b, (((1,), (1,)), ((), ())), preferred_element_type=F32)


def flip(index, bit):
    return index + bit - 2 * index * bit


def device_of(chip, other):
    ep, etp = lax.axis_index("ep"), lax.axis_index("etp")
    xb, yb = {OWN: (0, 0), DIAG: (1, 1), XN: (1, 0), YN: (0, 1)}[chip]
    return {"dp": lax.axis_index("dp"), "etp": flip(etp, yb), "ep": flip(ep // 2, xb) * 2 + flip(ep % 2, other)}


def rows_kernel(
    sizes, u_hbm, dy_hbm, ids_ref, wr_ref, wg_hbm, wu_hbm, wd_hbm,
    rows_out, ga_out, d1_out, d3_out, dl_out, own_out, send_out,
    ud, rt, w1, w3, w2, ga, d1, d3, ys, yo, yr, dgacc, dgb, dgr, dlb, wr16,
    in_sem, w_sem, ag_send, ag_recv, small_send, small_recv, pair_send, pair_recv, out_sem,
):
    tok, d_model, ffn, local_exp, experts, top_k = sizes
    half = tok // 2
    ep = lax.axis_index("ep")

    load_rows = [pltpu.make_async_copy(src, ud.at[k, pl.ds(0, tok), :], in_sem.at[k]) for k, src in enumerate((u_hbm, dy_hbm))]
    for c in load_rows:
        c.start()

    def load_w(e):
        cols = pl.ds(pl.multiple_of(e * ffn, ffn), ffn)
        return [
            pltpu.make_async_copy(wg_hbm.at[e], w1.at[:, cols], w_sem.at[0, e]),
            pltpu.make_async_copy(wu_hbm.at[e], w3.at[:, cols], w_sem.at[1, e]),
            pltpu.make_async_copy(wd_hbm.at[e], w2.at[cols, :], w_sem.at[2, e]),
        ]

    for e in range(local_exp):
        for c in load_w(e):
            c.start()

    barrier = pltpu.get_barrier_semaphore()
    others = [(chip, o) for chip in (OWN, DIAG, XN, YN) for o in (0, 1) if (chip, o) != (OWN, 0)]
    for chip, o in others:
        pl.semaphore_signal(barrier, inc=1, device_id=device_of(chip, o), device_id_type=MESH)

    lane40 = lax.broadcasted_iota(jnp.int32, (experts, LANES), 1) % 64
    row40 = lax.broadcasted_iota(jnp.int32, (experts, LANES), 0)
    spread = (row40 == (lane40 // GROUP) * local_exp + lane40 % GROUP) & (lane40 % GROUP < local_exp)
    wr16[...] = dot(wr_ref[...], jnp.where(spread, 1.0, 0.0).astype(BF16)).astype(BF16)
    for c in load_rows:
        c.wait()
    logits = dot(ud[0, 0:tok, :], wr16[...])
    lane = lax.broadcasted_iota(jnp.int32, (tok, LANES), 1)
    slot = lane % 64
    valid = slot % GROUP < local_exp
    logits = jnp.where(valid, logits, -1e30)
    top = jnp.max(logits, axis=1, keepdims=True)
    expo = jnp.where(valid, jnp.exp(logits - top), 0.0)
    prob = expo / jnp.sum(jnp.where(lane < 64, expo, 0.0), axis=1, keepdims=True)
    expert_of = jnp.where(valid, (slot // GROUP) * local_exp + slot % GROUP, -1)
    chosen = jnp.zeros((tok, LANES), jnp.bool_)
    ids = ids_ref[...]
    for j in range(top_k):
        chosen = chosen | (ids[:, j : j + 1] == expert_of)
    rt[0:tok, :] = jnp.where((lane < 64) | chosen, prob, -1.0)

    pl.semaphore_wait(barrier, len(others))

    def gather_copies(i, src, dst, count, dev):
        return [
            pltpu.make_async_remote_copy(rt.at[pl.ds(src, count), :], rt.at[pl.ds(dst, count), :], ag_send.at[0, i], ag_recv.at[0, i], device_id=dev, device_id_type=MESH),
            pltpu.make_async_remote_copy(ud.at[:, pl.ds(src, count), :], ud.at[:, pl.ds(dst, count), :], ag_send.at[1, i], ag_recv.at[1, i], device_id=dev, device_id_type=MESH),
        ]

    def xy_row(p, k):
        return 4 * tok + 2 * tok * p + half * k

    partner = device_of(OWN, 1)
    to_partner = gather_copies(0, 0, tok, tok, partner)
    to_x = [gather_copies(1 + p, half * p, xy_row(p, 0), half, device_of(XN, 0)) for p in (0, 1)]
    to_y = [gather_copies(3 + p, half * p, xy_row(p, 2), half, device_of(YN, 0)) for p in (0, 1)]
    to_d = gather_copies(5, 0, 2 * tok, tok, device_of(DIAG, 0))
    fwd_x = [gather_copies(6 + p, xy_row(p, 0), xy_row(p, 1), half, partner) for p in (0, 1)]
    fwd_y = [gather_copies(8 + p, xy_row(p, 2), xy_row(p, 3), half, partner) for p in (0, 1)]
    fwd_d = gather_copies(10, 2 * tok, 3 * tok, tok, partner)

    def start(copies):
        for c in copies:
            c.start()

    def wait_recv(copies):
        for c in copies:
            c.wait_recv()

    start(to_partner)
    for p in (0, 1):
        start(to_x[p])
        start(to_y[p])
    start(to_d)

    def expert_rows(row, e):
        rows = pl.ds(row, 2 * tok)
        cols = pl.ds(pl.multiple_of(e * ffn, ffn), ffn)
        h1 = dot(ud[0, rows, :], w1[:, cols]).astype(BF16).astype(F32)
        h3 = dot(ud[0, rows, :], w3[:, cols]).astype(BF16).astype(F32)
        da = dot_t(ud[1, rows, :], w2[cols, :])
        lanes = lax.broadcasted_iota(jnp.int32, (2 * tok, LANES), 1)
        mine = lanes == ep * GROUP + e
        gate = jnp.sum(jnp.where(lanes == 64 + ep * GROUP + e, rt[rows, :], 0.0), axis=1, keepdims=True)
        on = gate >= 0.0
        sig = jax.nn.sigmoid(h1)
        silu = h1 * sig
        act = (silu * h3).astype(BF16).astype(F32)
        ga[rows, cols] = jnp.where(on, gate * act, 0.0).astype(BF16)
        dgate = jnp.sum(act * da, axis=1, keepdims=True)
        dgacc[...] = jnp.where(mine, dgate, dgacc[...])
        da = (gate * da).astype(BF16).astype(F32)
        d1[rows, cols] = jnp.where(on, da * h3 * sig * (1.0 + h1 * (1.0 - sig)), 0.0).astype(BF16)
        d3[rows, cols] = jnp.where(on, da * silu, 0.0).astype(BF16)

    def rows_pass(row, first=False):
        dgacc[...] = jnp.zeros_like(dgacc)

        def body(i, carry):
            for k in range(2):
                if first:
                    for c in load_w(2 * i + k):
                        c.wait()
            for k in range(2):
                expert_rows(row, 2 * i + k)
            return carry

        lax.fori_loop(0, local_exp // 2, body, 0)

    outs = []

    def write_out(row):
        i = row // (2 * tok)
        rows = pl.ds(row, 2 * tok)
        copies = [pltpu.make_async_copy(s.at[rows, :], d.at[rows, :], out_sem.at[k, i]) for k, (s, d) in enumerate(((ga, ga_out), (d1, d1_out), (d3, d3_out)))]
        copies.append(pltpu.make_async_copy(ud.at[:, rows, :], rows_out.at[:, rows, :], out_sem.at[3, i]))
        start(copies)
        outs.extend(copies)

    def small(i, src, dst, dev):
        return pltpu.make_async_remote_copy(src, dst, small_send.at[i], small_recv.at[i], device_id=dev, device_id_type=MESH)

    dg_copies = {(chip, o): small(2 * chip + o, dgb.at[2 * chip + o], dgr.at[2 * chip + o], device_of(chip, o)) for chip, o in others}
    dl_copies = {(chip, o): small(8 + 2 * chip + o, dlb.at[0], dlb.at[2 * chip + o], device_of(chip, o)) for chip, o in others}

    to_partner[0].wait_recv()
    to_partner[1].wait_recv()
    rows_pass(0, first=True)
    write_out(0)
    dgb[0] = dgacc[0:tok, :]
    dgb[1] = dgacc[tok : 2 * tok, :]
    dg_copies[(OWN, 1)].start()

    for p in (0, 1):
        wait_recv(to_x[p])
        start(fwd_x[p])
        wait_recv(to_y[p])
        start(fwd_y[p])
        wait_recv(fwd_x[p])
        wait_recv(fwd_y[p])
        rows_pass(4 * tok + 2 * tok * p)
        write_out(4 * tok + 2 * tok * p)
        for k in range(4):
            dgb[4 + k, half * p : half * (p + 1), :] = dgacc[half * k : half * (k + 1), :]
    for chip in (XN, YN):
        for o in (0, 1):
            dg_copies[(chip, o)].start()

    def store_xy(k, tile, cols):
        for p in (0, 1):
            for c in (0, 1):
                at = 2 * tok * p + 2 * half * c
                ys[XN + c, k, half * p : half * (p + 1), cols] = tile[at : at + half]
                yo[XN + c, k, half * p : half * (p + 1), cols] = tile[at + half : at + 2 * half].astype(BF16)

    def store_own(k, tile, cols):
        for c in (0, 1):
            at = 2 * tok * c
            ys[OWN + c, k, :, cols] = tile[at : at + tok]
            yo[OWN + c, k, :, cols] = tile[at + tok : at + 2 * tok].astype(BF16)

    def sums_pass(row, store, lo, hi):
        rows = pl.ds(row, 4 * tok)
        width = 256

        def body(n, carry):
            cols = pl.ds(pl.multiple_of(n * width, width), width)
            store(0, dot(ga[rows, :], w2[:, cols]), cols)
            store(1, dot_t(d1[rows, :], w1[cols, :]) + dot_t(d3[rows, :], w3[cols, :]), cols)
            return carry

        lax.fori_loop(lo, hi, body, 0)

    pair = [
        pltpu.make_async_remote_copy(yo.at[pl.ds(2 * i, 2)], yr.at[pl.ds(2 * i, 2)], pair_send.at[i], pair_recv.at[i], device_id=partner, device_id_type=MESH)
        for i in (0, 1)
    ]
    steps = d_model // 256
    sums_pass(4 * tok, store_xy, 0, steps)
    pair[1].start()

    wait_recv(to_d)
    start(fwd_d)
    wait_recv(fwd_d)
    rows_pass(2 * tok)
    write_out(2 * tok)
    dgb[2] = dgacc[0:tok, :]
    dgb[3] = dgacc[tok : 2 * tok, :]
    for o in (0, 1):
        dg_copies[(DIAG, o)].start()
    sums_pass(0, store_own, 0, steps // 2)

    for c in dg_copies.values():
        c.wait_recv()
    dgate = dgb[0]
    for chip, o in others:
        dgate = dgate + dgr[2 * chip + o]
    own_rt = rt[0:tok, :]
    left = lane < 64
    prob = jnp.where(left, own_rt, 0.0)
    dprob = jnp.where(left & (pltpu.roll(own_rt, 64, 1) >= 0.0), dgate, 0.0)
    dlogit = prob * (dprob - jnp.sum(prob * dprob, axis=1, keepdims=True))
    high = dlogit.astype(BF16)
    low = dlogit - high.astype(F32)
    dlb[0] = jnp.where(left, high.astype(F32), pltpu.roll(low, 64, 1)).astype(BF16)
    for c in dl_copies.values():
        c.start()

    sums_pass(0, store_own, steps // 2, steps)
    pair[0].start()
    du_router = dot_t(dlb[0], wr16[...])

    pair[1].wait_recv()
    for k in (0, 1):
        send_out[1, k] = (ys[XN, k] + yr[XN, k].astype(F32)).astype(BF16)
        send_out[2, k] = (ys[YN, k] + yr[YN, k].astype(F32)).astype(BF16)
    for c in dl_copies.values():
        c.wait_recv()
    dl_out[0 : 2 * tok, :] = dlb[0:2].reshape(2 * tok, LANES)
    dl_out[2 * tok : 4 * tok, :] = dlb[2:4].reshape(2 * tok, LANES)
    for p in (0, 1):
        for k in range(4):
            at = 4 * tok + 2 * tok * p + half * k
            dl_out[at : at + half, :] = dlb[4 + k, half * p : half * (p + 1), :]
    pair[0].wait_recv()
    for k in (0, 1):
        send_out[0, k] = (ys[DIAG, k] + yr[DIAG, k].astype(F32)).astype(BF16)
    own_out[0] = ys[OWN, 0] + yr[OWN, 0].astype(F32) + ud[0, 0:tok, :].astype(F32)
    own_out[1] = ys[OWN, 1] + yr[OWN, 1].astype(F32) + ud[1, 0:tok, :].astype(F32) + du_router

    for copies in (to_partner, *to_x, *to_y, to_d, *fwd_x, *fwd_y, fwd_d):
        for c in copies:
            c.wait_send()
    for c in (*dg_copies.values(), *dl_copies.values(), *pair):
        c.wait_send()
    for c in outs:
        c.wait()


def grads_kernel(local_exp, rows_ref, ga_ref, d1_ref, d3_ref, dl_ref, dwg_ref, dwu_ref, dwd_ref, dwr_ref, xt):
    @pl.when(pl.program_id(0) == 0)
    def _():
        xt[...] = rows_ref[0].T
        wide = dot(xt[...], dl_ref[...])
        wide = wide + pltpu.roll(wide, 64, 1)
        lane = lax.broadcasted_iota(jnp.int32, wide.shape, 1)
        out = wide
        for g in range(1, dwr_ref.shape[1] // local_exp):
            out = jnp.where(lane >= g * local_exp, pltpu.roll(wide, LANES - g * (GROUP - local_exp), 1), out)
        dwr_ref[...] = out[:, : dwr_ref.shape[1]]

    dwg_ref[0] = dot(xt[...], d1_ref[...])
    dwu_ref[0] = dot(xt[...], d3_ref[...])
    dwd_ref[0] = lax.dot_general(ga_ref[...], rows_ref[1], (((0,), (0,)), ((), ())), preferred_element_type=F32)


def solution(mesh):
    tok_spec = P(("dp", "ep", "etp"), None)
    col_spec = P("ep", None, "etp")
    row_spec = P("ep", "etp", None)
    in_specs = (tok_spec, tok_spec, tok_spec, P(None, None), col_spec, col_spec, row_spec)
    out_specs = (tok_spec, tok_spec, P(("dp", "ep"), None, "etp"), P(("dp", "ep"), None, "etp"), P(("dp", "ep"), "etp", None), P("dp", None))

    def device_step(u_loc, dy_loc, ids_loc, w_router, w_gate, w_up, w_down):
        tok, d_model = u_loc.shape
        top_k = ids_loc.shape[1]
        experts = w_router.shape[1]
        local_exp, _, ffn = w_gate.shape
        rows = 8 * tok
        wide = local_exp * ffn
        any_spec = pl.BlockSpec(memory_space=pl.ANY)
        vmem_spec = pl.BlockSpec(memory_space=pltpu.VMEM)
        S = jax.ShapeDtypeStruct
        ud, ga, d1, d3, dl, own, send = pl.pallas_call(
            functools.partial(rows_kernel, (tok, d_model, ffn, local_exp, experts, top_k)),
            name="expert_rows",
            in_specs=[any_spec, any_spec, vmem_spec, vmem_spec, any_spec, any_spec, any_spec],
            out_specs=[any_spec] * 4 + [vmem_spec] * 3,
            out_shape=[
                S((2, rows, d_model), BF16), S((rows, wide), BF16), S((rows, wide), BF16), S((rows, wide), BF16),
                S((rows, LANES), BF16), S((2, tok, d_model), F32), S((3, 2, tok, d_model), BF16),
            ],
            scratch_shapes=[
                pltpu.VMEM((2, rows, d_model), BF16),
                pltpu.VMEM((rows, LANES), F32),
                pltpu.VMEM((d_model, wide), BF16), pltpu.VMEM((d_model, wide), BF16), pltpu.VMEM((wide, d_model), BF16),
                pltpu.VMEM((rows, wide), BF16), pltpu.VMEM((rows, wide), BF16), pltpu.VMEM((rows, wide), BF16),
                pltpu.VMEM((4, 2, tok, d_model), F32),
                pltpu.VMEM((4, 2, tok, d_model), BF16), pltpu.VMEM((4, 2, tok, d_model), BF16),
                pltpu.VMEM((2 * tok, LANES), F32),
                pltpu.VMEM((8, tok, LANES), F32), pltpu.VMEM((8, tok, LANES), F32),
                pltpu.VMEM((8, tok, LANES), BF16),
                pltpu.VMEM((d_model, LANES), BF16),
                pltpu.SemaphoreType.DMA((2,)), pltpu.SemaphoreType.DMA((3, local_exp)),
                pltpu.SemaphoreType.DMA((2, 11)), pltpu.SemaphoreType.DMA((2, 11)),
                pltpu.SemaphoreType.DMA((16,)), pltpu.SemaphoreType.DMA((16,)),
                pltpu.SemaphoreType.DMA((2,)), pltpu.SemaphoreType.DMA((2,)),
                pltpu.SemaphoreType.DMA((4, 4)),
            ],
            compiler_params=pltpu.CompilerParams(collective_id=0, has_side_effects=True, vmem_limit_bytes=62 * 1024 * 1024),
        )(u_loc, dy_loc, ids_loc, w_router, w_gate, w_up, w_down)

        n_ep, n_etp = lax.axis_size("ep"), lax.axis_size("etp")
        got_x = lax.ppermute(send[1], "ep", [(i, i ^ 2) for i in range(n_ep)])
        got_y = lax.ppermute(send[2], "etp", [(i, i ^ 1) for i in range(n_etp)])
        got_d = lax.ppermute(send[0], ("etp", "ep"), [(i, i ^ (n_ep + 2)) for i in range(n_ep * n_etp)])

        col_block = pl.BlockSpec((rows, ffn), lambda e: (0, e))
        dwg, dwu, dwd, dwr = pl.pallas_call(
            functools.partial(grads_kernel, local_exp),
            name="weight_grads",
            grid=(local_exp,),
            in_specs=[
                pl.BlockSpec((2, rows, d_model), lambda e: (0, 0, 0)),
                col_block, col_block, col_block,
                pl.BlockSpec((rows, LANES), lambda e: (0, 0)),
            ],
            out_specs=[
                pl.BlockSpec((1, d_model, ffn), lambda e: (e, 0, 0)),
                pl.BlockSpec((1, d_model, ffn), lambda e: (e, 0, 0)),
                pl.BlockSpec((1, ffn, d_model), lambda e: (e, 0, 0)),
                pl.BlockSpec((d_model, experts), lambda e: (0, 0)),
            ],
            out_shape=[S((local_exp, d_model, ffn), F32), S((local_exp, d_model, ffn), F32), S((local_exp, ffn, d_model), F32), S((d_model, experts), F32)],
            scratch_shapes=[pltpu.VMEM((d_model, rows), BF16)],
            compiler_params=pltpu.CompilerParams(vmem_limit_bytes=48 * 1024 * 1024),
            cost_estimate=pl.CostEstimate(flops=3 * 2 * rows * wide * d_model, bytes_accessed=12 * wide * d_model + 10 * rows * wide, transcendentals=0),
        )(ud, ga, d1, d3, dl)

        total = own + got_x.astype(F32) + got_y.astype(F32) + got_d.astype(F32)
        return total[0].astype(BF16), total[1].astype(BF16), dwg, dwu, dwd, dwr

    return jax.shard_map(device_step, mesh=mesh, in_specs=in_specs, out_specs=out_specs, check_vma=False)
```

```python
import functools

import jax
import jax.numpy as jnp
from jax import lax
from jax.experimental import pallas as pl
from jax.experimental.pallas import tpu as pltpu
from jax.sharding import PartitionSpec as P

MESH = pl.DeviceIdType.MESH
F32 = jnp.float32
BF16 = jnp.bfloat16
LANES = 128
GROUP = 16
OWN, DIAG, XN, YN = 0, 1, 2, 3


def dot(a, b):
    return jnp.dot(a, b, preferred_element_type=F32)


def dot_t(a, b):
    return lax.dot_general(a, b, (((1,), (1,)), ((), ())), preferred_element_type=F32)


def flip(index, bit):
    return index + bit - 2 * index * bit


def device_of(chip, other):
    ep, etp = lax.axis_index("ep"), lax.axis_index("etp")
    xb, yb = {OWN: (0, 0), DIAG: (1, 1), XN: (1, 0), YN: (0, 1)}[chip]
    return {"dp": lax.axis_index("dp"), "etp": flip(etp, yb), "ep": flip(ep // 2, xb) * 2 + flip(ep % 2, other)}


def rows_kernel(
    sizes, u_hbm, dy_hbm, ids_ref, wr_ref, wg_hbm, wu_hbm, wd_hbm,
    u_out, dy_out, ga_out, d1_out, d3_out, dl_out, own_out, send_out,
    u, dy, rt, w1, w3, w2, ga, d1, d3, sg, ys, yo, yr, xs, xr, dgacc, dgb, dgr, dlb, wr16,
    in_sem, w_sem, ag_send, ag_recv, small_send, small_recv, pair_send, pair_recv, xy_send, xy_recv, out_sem,
):
    tok, d_model, ffn, local_exp, experts, top_k = sizes
    ep = lax.axis_index("ep")

    load_rows = [pltpu.make_async_copy(src, dst.at[pl.ds(0, tok), :], in_sem.at[k]) for k, (src, dst) in enumerate(((u_hbm, u), (dy_hbm, dy)))]
    for c in load_rows:
        c.start()

    def load_w(e):
        cols = pl.ds(pl.multiple_of(e * ffn, ffn), ffn)
        return [
            pltpu.make_async_copy(wg_hbm.at[e], w1.at[:, cols], w_sem.at[0, e]),
            pltpu.make_async_copy(wu_hbm.at[e], w3.at[:, cols], w_sem.at[1, e]),
            pltpu.make_async_copy(wd_hbm.at[e], w2.at[cols, :], w_sem.at[2, e]),
        ]

    barrier = pltpu.get_barrier_semaphore()
    others = [(chip, o) for chip in (OWN, DIAG, XN, YN) for o in (0, 1) if (chip, o) != (OWN, 0)]
    for chip, o in others:
        pl.semaphore_signal(barrier, inc=1, device_id=device_of(chip, o), device_id_type=MESH)

    slot40 = lax.broadcasted_iota(jnp.int32, (LANES, experts), 0) % 64
    col40 = lax.broadcasted_iota(jnp.int32, (LANES, experts), 1)
    spread = (col40 == (slot40 // GROUP) * local_exp + slot40 % GROUP) & (slot40 % GROUP < local_exp)
    wr16[...] = dot(jnp.where(spread, 1.0, 0.0).astype(BF16), wr_ref[...]).astype(BF16)
    slot_t = lax.broadcasted_iota(jnp.int32, (LANES, tok), 0) % 64
    expert_t = jnp.where(slot_t % GROUP < local_exp, (slot_t // GROUP) * local_exp + slot_t % GROUP, -1)
    chosen_t = jnp.zeros((LANES, tok), F32)
    for j in range(top_k):
        chosen_t = jnp.where(expert_t == ids_ref[j : j + 1, :], 1.0, chosen_t)
    chosen = chosen_t.T > 0.5
    lane = lax.broadcasted_iota(jnp.int32, (tok, LANES), 1)
    valid = lane % GROUP < local_exp
    for c in load_rows:
        c.wait()
    for which in (slice(0, 2), slice(2, 3)):
        for e in range(local_exp):
            for c in load_w(e)[which]:
                c.start()

    logits = jnp.where(valid, dot_t(u[0:tok, :], wr16[...]), -1e30)
    top = jnp.max(logits, axis=1, keepdims=True)
    expo = jnp.where(valid, jnp.exp(logits - top), 0.0)
    prob = expo / jnp.sum(jnp.where(lane < 64, expo, 0.0), axis=1, keepdims=True)
    rt[0:tok, :] = jnp.where((lane < 64) | chosen, prob, -1.0)

    pl.semaphore_wait(barrier, len(others))

    def block(chip, o):
        return pl.ds((2 * chip + o) * tok, tok)

    def gather(i, src, dst, dev):
        return [
            pltpu.make_async_remote_copy(ref.at[src, :], ref.at[dst, :], ag_send.at[k, i], ag_recv.at[k, i], device_id=dev, device_id_type=MESH)
            for k, ref in enumerate((rt, u, dy))
        ]

    partner = device_of(OWN, 1)
    to_partner = gather(0, block(OWN, 0), block(OWN, 1), partner)
    to_chip = {chip: gather(chip, block(OWN, 0), block(chip, 0), device_of(chip, 0)) for chip in (DIAG, XN, YN)}
    forward = {chip: gather(3 + chip, block(chip, 0), block(chip, 1), partner) for chip in (DIAG, XN, YN)}

    def start(copies):
        for c in copies:
            c.start()

    def wait_recv(copies):
        for c in copies:
            c.wait_recv()

    def send_part(k):
        for copies in (to_partner, to_chip[XN], to_chip[YN]):
            copies[k].start()

    send_part(0)
    send_part(1)

    def pass_on(chip, parts):
        for k in parts:
            to_chip[chip][k].wait_recv()
            forward[chip][k].start()

    def cols_of(e):
        return pl.ds(pl.multiple_of(e * ffn, ffn), ffn)

    def gate_of(rows, count, e):
        lanes = lax.broadcasted_iota(jnp.int32, (count, LANES), 1)
        return jnp.sum(jnp.where(lanes == 64 + ep * GROUP + e, rt[rows, :], 0.0), axis=1, keepdims=True)

    unroll = 5

    def over_experts(lo, hi, one, which=None):
        def body(i, carry):
            if which is not None:
                for k in range(unroll):
                    for c in load_w(i * unroll + k)[which]:
                        c.wait()
            for k in range(unroll):
                one(i * unroll + k)
            return carry

        lax.fori_loop(lo // unroll, hi // unroll, body, 0)

    def u_pass(row, count, lo, hi, first=False):
        rows = pl.ds(row, count)

        def one(e):
            cols = cols_of(e)
            h1 = dot(u[rows, :], w1[:, cols]).astype(BF16)
            h3 = dot(u[rows, :], w3[:, cols]).astype(BF16)
            d1[rows, cols] = h1
            d3[rows, cols] = h3
            gate = gate_of(rows, count, e)
            h1 = h1.astype(F32)
            sig = jax.nn.sigmoid(h1)
            sg[rows, cols] = sig
            act = (h1 * sig * h3.astype(F32)).astype(BF16).astype(F32)
            ga[rows, cols] = jnp.where(gate >= 0.0, gate * act, 0.0).astype(BF16)

        over_experts(lo, hi, one, slice(0, 2) if first else None)

    def dy_pass(row, count, first=False):
        rows = pl.ds(row, count)

        def one(e):
            cols = cols_of(e)
            da = dot_t(dy[rows, :], w2[cols, :])
            lanes = lax.broadcasted_iota(jnp.int32, (count, LANES), 1)
            gate = gate_of(rows, count, e)
            on = gate >= 0.0
            h1 = d1[rows, cols].astype(F32)
            h3 = d3[rows, cols].astype(F32)
            sig = sg[rows, cols]
            silu = h1 * sig
            act = (silu * h3).astype(BF16).astype(F32)
            dgate = jnp.sum(act * da, axis=1, keepdims=True)
            dgacc[...] = jnp.where(lanes == ep * GROUP + e, dgate, dgacc[...])
            da = (gate * da).astype(BF16).astype(F32)
            d1[rows, cols] = jnp.where(on, da * (h3 * (sig * (1.0 + h1 * (1.0 - sig)))), 0.0).astype(BF16)
            d3[rows, cols] = jnp.where(on, da * silu, 0.0).astype(BF16)

        dgacc[...] = jnp.zeros_like(dgacc)
        over_experts(0, local_exp, one, slice(2, 3) if first else None)

    outs = []

    def write_out(row, count, pairs, sem):
        rows = pl.ds(row, count)
        copies = [pltpu.make_async_copy(s.at[rows, :], d.at[rows, :], out_sem.at[sem, k]) for k, (s, d) in enumerate(pairs)]
        start(copies)
        outs.extend(copies)

    grads = ((ga, ga_out), (d1, d1_out), (d3, d3_out), (u, u_out), (dy, dy_out))

    def small(i, src, dst, dev):
        return pltpu.make_async_remote_copy(src, dst, small_send.at[i], small_recv.at[i], device_id=dev, device_id_type=MESH)

    dg_copies = {(chip, o): small(2 * chip + o, dgb.at[2 * chip + o], dgr.at[2 * chip + o], device_of(chip, o)) for chip, o in others}
    dl_copies = {(chip, o): small(8 + 2 * chip + o, dlb.at[0], dlb.at[2 * chip + o], device_of(chip, o)) for chip, o in others}

    def send_gates(chips):
        for i, chip in enumerate(chips):
            for o in (0, 1):
                k = 2 * i + o
                dgb[2 * chip + o] = dgacc[k * tok : (k + 1) * tok, :]
                if (chip, o) != (OWN, 0):
                    dg_copies[(chip, o)].start()

    def sums_pass(row, chips, lo, hi):
        rows = pl.ds(row, 4 * tok)
        width = 256
        for n in range(lo, hi):
            cols = pl.ds(n * width, width)
            y = dot(ga[rows, :], w2[:, cols])
            dx = dot_t(d1[rows, :], w1[cols, :]) + dot_t(d3[rows, :], w3[cols, :])
            for k, tile in enumerate((y, dx)):
                for i, chip in enumerate(chips):
                    at = 2 * tok * i
                    ys[chip, k, :, cols] = tile[at : at + tok]
                    yo[chip, k, :, cols] = tile[at + tok : at + 2 * tok].astype(BF16)

    pair = [
        pltpu.make_async_remote_copy(yo.at[pl.ds(2 * i, 2)], yr.at[pl.ds(2 * i, 2)], pair_send.at[i], pair_recv.at[i], device_id=partner, device_id_type=MESH)
        for i in (0, 1)
    ]
    xy = [
        pltpu.make_async_remote_copy(xs.at[i], xr.at[i], xy_send.at[i], xy_recv.at[i], device_id=device_of(chip, 0), device_id_type=MESH)
        for i, chip in enumerate((XN, YN))
    ]
    steps = d_model // 256

    wait_recv(to_partner[:2])
    u_pass(0, 2 * tok, 0, local_exp, first=True)
    send_part(2)

    for chip in (XN, YN):
        pass_on(chip, (0, 1))
    for chip in (XN, YN):
        wait_recv(forward[chip][:2])
    u_pass(4 * tok, 4 * tok, 0, unroll)
    start(to_chip[DIAG])
    for chip in (XN, YN):
        pass_on(chip, (2,))
    u_pass(4 * tok, 4 * tok, unroll, local_exp)
    for chip in (XN, YN):
        forward[chip][2].wait_recv()
    dy_pass(4 * tok, 4 * tok, first=True)
    write_out(4 * tok, 4 * tok, grads, 0)
    send_gates((XN, YN))
    sums_pass(4 * tok, (XN, YN), 0, steps - 2)
    pass_on(DIAG, (0, 1, 2))
    sums_pass(4 * tok, (XN, YN), steps - 2, steps)
    pair[1].start()

    wait_recv(forward[DIAG])
    to_partner[2].wait_recv()
    u_pass(2 * tok, 2 * tok, 0, local_exp)
    pair[1].wait_recv()
    for i, chip in enumerate((XN, YN)):
        for k in (0, 1):
            xs[i, k] = (ys[chip, k] + yr[chip, k].astype(F32)).astype(BF16)
        xy[i].start()
    dy_pass(0, 4 * tok)
    write_out(0, 4 * tok, grads, 1)
    send_gates((OWN, DIAG))
    sums_pass(0, (OWN, DIAG), 0, steps - 2)

    for c in dg_copies.values():
        c.wait_recv()
    dgate = dgb[0]
    for chip, o in others:
        dgate = dgate + dgr[2 * chip + o]
    own_rt = rt[0:tok, :]
    left = lane < 64
    prob = jnp.where(left, own_rt, 0.0)
    dprob = jnp.where(left & (pltpu.roll(own_rt, 64, 1) >= 0.0), dgate, 0.0)
    dlogit = prob * (dprob - jnp.sum(prob * dprob, axis=1, keepdims=True))
    high = dlogit.astype(BF16)
    low = dlogit - high.astype(F32)
    dlb[0] = jnp.where(left, high.astype(F32), pltpu.roll(low, 64, 1)).astype(BF16)
    start(dl_copies.values())

    sums_pass(0, (OWN, DIAG), steps - 2, steps)
    pair[0].start()
    du_router = dot(dlb[0], wr16[...])
    wait_recv(dl_copies.values())
    dl_out[...] = dlb[...].reshape(8 * tok, LANES)
    pair[0].wait_recv()
    for k in (0, 1):
        send_out[k] = (ys[DIAG, k] + yr[DIAG, k].astype(F32)).astype(BF16)
    wait_recv(xy)
    for k, base in enumerate((u[0:tok, :].astype(F32), dy[0:tok, :].astype(F32) + du_router)):
        own_out[k] = ys[OWN, k] + yr[OWN, k].astype(F32) + base + xr[0, k].astype(F32) + xr[1, k].astype(F32)

    for copies in (to_partner, *to_chip.values(), *forward.values(), dg_copies.values(), dl_copies.values(), pair, xy):
        for c in copies:
            c.wait_send()
    for c in outs:
        c.wait()


def grads_kernel(local_exp, u_ref, dy_ref, ga_ref, d1_ref, d3_ref, dl_ref, dwg_ref, dwu_ref, dwd_ref, dwr_ref, xt):
    def over_tokens(a, b):
        return lax.dot_general(a, b, (((0,), (0,)), ((), ())), preferred_element_type=F32)

    @pl.when(pl.program_id(0) == 0)
    def _():
        xt[...] = u_ref[...].T
        wide = over_tokens(dl_ref[...], u_ref[...])
        wide = wide[0:64] + wide[64:128]
        for g in range(dwr_ref.shape[0] // local_exp):
            dwr_ref[g * local_exp : (g + 1) * local_exp, :] = wide[g * GROUP : g * GROUP + local_exp]

    dwg_ref[0] = dot(xt[...], d1_ref[...])
    dwu_ref[0] = dot(xt[...], d3_ref[...])
    dwd_ref[0] = over_tokens(ga_ref[...], dy_ref[...])


def solution(mesh):
    tok_spec = P(("dp", "ep", "etp"), None)
    col_spec = P("ep", None, "etp")
    row_spec = P("ep", "etp", None)
    in_specs = (tok_spec, tok_spec, tok_spec, P(None, None), col_spec, col_spec, row_spec)
    out_specs = (tok_spec, tok_spec, P(("dp", "ep"), None, "etp"), P(("dp", "ep"), None, "etp"), P(("dp", "ep"), "etp", None), P("dp", None))

    def device_step(u_loc, dy_loc, ids_loc, w_router, w_gate, w_up, w_down):
        tok, d_model = u_loc.shape
        top_k = ids_loc.shape[1]
        experts = w_router.shape[1]
        local_exp, _, ffn = w_gate.shape
        rows = 8 * tok
        wide = local_exp * ffn
        any_spec = pl.BlockSpec(memory_space=pl.ANY)
        vmem_spec = pl.BlockSpec(memory_space=pltpu.VMEM)
        S = jax.ShapeDtypeStruct
        dma = pltpu.SemaphoreType.DMA
        u, dy, ga, d1, d3, dl, own, send = pl.pallas_call(
            functools.partial(rows_kernel, (tok, d_model, ffn, local_exp, experts, top_k)),
            name="expert_rows",
            in_specs=[any_spec, any_spec, vmem_spec, vmem_spec, any_spec, any_spec, any_spec],
            out_specs=[any_spec] * 5 + [vmem_spec] * 3,
            out_shape=[
                S((rows, d_model), BF16), S((rows, d_model), BF16),
                S((rows, wide), BF16), S((rows, wide), BF16), S((rows, wide), BF16),
                S((rows, LANES), BF16), S((2, tok, d_model), F32), S((2, tok, d_model), BF16),
            ],
            scratch_shapes=[
                pltpu.VMEM((rows, d_model), BF16), pltpu.VMEM((rows, d_model), BF16),
                pltpu.VMEM((rows, LANES), F32),
                pltpu.VMEM((d_model, wide), BF16), pltpu.VMEM((d_model, wide), BF16), pltpu.VMEM((wide, d_model), BF16),
                pltpu.VMEM((rows, wide), BF16), pltpu.VMEM((rows, wide), BF16), pltpu.VMEM((rows, wide), BF16), pltpu.VMEM((rows, wide), F32),
                pltpu.VMEM((4, 2, tok, d_model), F32),
                pltpu.VMEM((4, 2, tok, d_model), BF16), pltpu.VMEM((4, 2, tok, d_model), BF16),
                pltpu.VMEM((2, 2, tok, d_model), BF16), pltpu.VMEM((2, 2, tok, d_model), BF16),
                pltpu.VMEM((4 * tok, LANES), F32),
                pltpu.VMEM((8, tok, LANES), F32), pltpu.VMEM((8, tok, LANES), F32),
                pltpu.VMEM((8, tok, LANES), BF16),
                pltpu.VMEM((LANES, d_model), BF16),
                dma((2,)), dma((3, local_exp)), dma((3, 7)), dma((3, 7)), dma((16,)), dma((16,)),
                dma((2,)), dma((2,)), dma((2,)), dma((2,)), dma((2, 5)),
            ],
            compiler_params=pltpu.CompilerParams(collective_id=0, has_side_effects=True, vmem_limit_bytes=62 * 1024 * 1024),
        )(u_loc, dy_loc, ids_loc.T, w_router.T, w_gate, w_up, w_down)

        n_ep, n_etp = lax.axis_size("ep"), lax.axis_size("etp")
        got = lax.ppermute(send, ("etp", "ep"), [(i, i ^ (n_ep + 2)) for i in range(n_ep * n_etp)])

        col_block = pl.BlockSpec((rows, ffn), lambda e: (0, e))
        whole_rows = pl.BlockSpec((rows, d_model), lambda e: (0, 0))
        dwg, dwu, dwd, dwr = pl.pallas_call(
            functools.partial(grads_kernel, local_exp),
            name="weight_grads",
            grid=(local_exp,),
            in_specs=[whole_rows, whole_rows, col_block, col_block, col_block, pl.BlockSpec((rows, LANES), lambda e: (0, 0))],
            out_specs=[
                pl.BlockSpec((1, d_model, ffn), lambda e: (e, 0, 0)),
                pl.BlockSpec((1, d_model, ffn), lambda e: (e, 0, 0)),
                pl.BlockSpec((1, ffn, d_model), lambda e: (e, 0, 0)),
                pl.BlockSpec((experts, d_model), lambda e: (0, 0)),
            ],
            out_shape=[S((local_exp, d_model, ffn), F32), S((local_exp, d_model, ffn), F32), S((local_exp, ffn, d_model), F32), S((experts, d_model), F32)],
            scratch_shapes=[pltpu.VMEM((d_model, rows), BF16)],
            compiler_params=pltpu.CompilerParams(vmem_limit_bytes=62 * 1024 * 1024),
            cost_estimate=pl.CostEstimate(flops=3 * 2 * rows * wide * d_model, bytes_accessed=12 * wide * d_model + 10 * rows * wide, transcendentals=0),
        )(u, dy, ga, d1, d3, dl)

        y_loc = (own[0] + got[0].astype(F32)).astype(BF16)
        du_loc = (own[1] + got[1].astype(F32)).astype(BF16)
        return y_loc, du_loc, dwg, dwu, dwd, dwr.T

    return jax.shard_map(device_step, mesh=mesh, in_specs=in_specs, out_specs=out_specs, check_vma=False)
```

```python
import functools

import jax
import jax.numpy as jnp
from jax import lax
from jax.experimental import pallas as pl
from jax.experimental.pallas import tpu as pltpu
from jax.sharding import PartitionSpec as P

MESH = pl.DeviceIdType.MESH
F32 = jnp.float32
BF16 = jnp.bfloat16
LANES = 128
GROUP = 16
OWN, DIAG, XN, YN = 0, 1, 2, 3


def dot(a, b):
    return jnp.dot(a, b, preferred_element_type=F32)


def dot_t(a, b):
    return lax.dot_general(a, b, (((1,), (1,)), ((), ())), preferred_element_type=F32)


def flip(index, bit):
    return index + bit - 2 * index * bit


def device_of(chip, other):
    ep, etp = lax.axis_index("ep"), lax.axis_index("etp")
    xb, yb = {OWN: (0, 0), DIAG: (1, 1), XN: (1, 0), YN: (0, 1)}[chip]
    return {"dp": lax.axis_index("dp"), "etp": flip(etp, yb), "ep": flip(ep // 2, xb) * 2 + flip(ep % 2, other)}


def rows_kernel(
    sizes, u_hbm, dy_hbm, ids_ref, wr_ref, wg_hbm, wu_hbm, wd_hbm,
    u_out, dy_out, ga_out, d1_out, d3_out, dl_out, own_out, send_out,
    u, dy, rt, w1, w3, w2, ga, d1, d3, sg, ys, yo, yr, xs, xr, dgacc, dgb, dgr, dlb, wr16,
    in_sem, w_sem, ag_send, ag_recv, small_send, small_recv, pair_send, pair_recv, xy_send, xy_recv, out_sem,
):
    tok, d_model, ffn, local_exp, experts, top_k = sizes
    ep = lax.axis_index("ep")

    load_rows = [pltpu.make_async_copy(src, dst.at[pl.ds(0, tok), :], in_sem.at[k]) for k, (src, dst) in enumerate(((u_hbm, u), (dy_hbm, dy)))]
    for c in load_rows:
        c.start()

    def load_w(e):
        cols = pl.ds(pl.multiple_of(e * ffn, ffn), ffn)
        return [
            pltpu.make_async_copy(wg_hbm.at[e], w1.at[:, cols], w_sem.at[0, e]),
            pltpu.make_async_copy(wu_hbm.at[e], w3.at[:, cols], w_sem.at[1, e]),
            pltpu.make_async_copy(wd_hbm.at[e], w2.at[cols, :], w_sem.at[2, e]),
        ]

    barrier = pltpu.get_barrier_semaphore()
    others = [(chip, o) for chip in (OWN, DIAG, XN, YN) for o in (0, 1) if (chip, o) != (OWN, 0)]
    for chip, o in others:
        pl.semaphore_signal(barrier, inc=1, device_id=device_of(chip, o), device_id_type=MESH)

    slot40 = lax.broadcasted_iota(jnp.int32, (LANES, experts), 0) % 64
    col40 = lax.broadcasted_iota(jnp.int32, (LANES, experts), 1)
    spread = (col40 == (slot40 // GROUP) * local_exp + slot40 % GROUP) & (slot40 % GROUP < local_exp)
    wr16[...] = dot(jnp.where(spread, 1.0, 0.0).astype(BF16), wr_ref[...]).astype(BF16)
    slot_t = lax.broadcasted_iota(jnp.int32, (LANES, tok), 0) % 64
    expert_t = jnp.where(slot_t % GROUP < local_exp, (slot_t // GROUP) * local_exp + slot_t % GROUP, -1)
    chosen_t = jnp.zeros((LANES, tok), F32)
    for j in range(top_k):
        chosen_t = jnp.where(expert_t == ids_ref[j : j + 1, :], 1.0, chosen_t)
    chosen = chosen_t.T > 0.5
    lane = lax.broadcasted_iota(jnp.int32, (tok, LANES), 1)
    valid = lane % GROUP < local_exp
    for c in load_rows:
        c.wait()
    unroll = 5

    def start_w(lo, hi, which):
        for e in range(lo, hi):
            for c in load_w(e)[which]:
                c.start()

    start_w(0, unroll, slice(0, 2))

    logits = jnp.where(valid, dot_t(u[0:tok, :], wr16[...]), -1e30)
    top = jnp.max(logits, axis=1, keepdims=True)
    expo = jnp.where(valid, jnp.exp(logits - top), 0.0)
    prob = expo / jnp.sum(jnp.where(lane < 64, expo, 0.0), axis=1, keepdims=True)
    rt[0:tok, :] = jnp.where((lane < 64) | chosen, prob, -1.0)

    pl.semaphore_wait(barrier, len(others))
    start_w(unroll, local_exp, slice(0, 2))

    def block(chip, o):
        return pl.ds((2 * chip + o) * tok, tok)

    def gather(i, src, dst, dev):
        return [
            pltpu.make_async_remote_copy(ref.at[src, :], ref.at[dst, :], ag_send.at[k, i], ag_recv.at[k, i], device_id=dev, device_id_type=MESH)
            for k, ref in enumerate((rt, u, dy))
        ]

    partner = device_of(OWN, 1)
    to_partner = gather(0, block(OWN, 0), block(OWN, 1), partner)
    to_chip = {chip: gather(chip, block(OWN, 0), block(chip, 0), device_of(chip, 0)) for chip in (XN, YN)}
    forward = {chip: gather(3 + chip, block(chip, 0), block(chip, 1), partner) for chip in (DIAG, XN, YN)}
    half = tok // 2

    def half_of(chip, h):
        return pl.ds(2 * chip * tok + h * half, half)

    relay = {
        YN: gather(1, half_of(YN, 1), half_of(DIAG, 1), device_of(XN, 0)),
        XN: gather(7, half_of(XN, 0), half_of(DIAG, 0), device_of(YN, 0)),
    }

    def start(copies):
        for c in copies:
            c.start()

    def wait_recv(copies):
        for c in copies:
            c.wait_recv()

    for k in range(2):
        for copies in (to_partner, to_chip[XN], to_chip[YN]):
            copies[k].start()
    to_partner[2].start()

    def pass_on(parts):
        for chip in (XN, YN):
            for k in parts:
                to_chip[chip][k].wait_recv()
                relay[chip][k].start()
                forward[chip][k].start()

    def cols_of(e):
        return pl.ds(pl.multiple_of(e * ffn, ffn), ffn)

    def gate_of(rows, count, e):
        lanes = lax.broadcasted_iota(jnp.int32, (count, LANES), 1)
        return jnp.sum(jnp.where(lanes == 64 + ep * GROUP + e, rt[rows, :], 0.0), axis=1, keepdims=True)

    def over_experts(lo, hi, one, which=None):
        def body(i, carry):
            if which is not None:
                for k in range(unroll):
                    for c in load_w(i * unroll + k)[which]:
                        c.wait()
            for k in range(unroll):
                one(i * unroll + k)
            return carry

        lax.fori_loop(lo // unroll, hi // unroll, body, 0)

    def u_pass(row, count, lo, hi, first=False):
        rows = pl.ds(row, count)

        def one(e):
            cols = cols_of(e)
            h1 = dot(u[rows, :], w1[:, cols]).astype(BF16)
            h3 = dot(u[rows, :], w3[:, cols]).astype(BF16)
            d1[rows, cols] = h1
            d3[rows, cols] = h3
            gate = gate_of(rows, count, e)
            h1 = h1.astype(F32)
            sig = jax.nn.sigmoid(h1)
            sg[rows, cols] = sig
            act = (h1 * sig * h3.astype(F32)).astype(BF16).astype(F32)
            ga[rows, cols] = jnp.where(gate >= 0.0, gate * act, 0.0).astype(BF16)

        over_experts(lo, hi, one, slice(0, 2) if first else None)

    def dy_pass(row, count, lo, hi):
        rows = pl.ds(row, count)
        if lo == 0:
            dgacc[...] = jnp.zeros_like(dgacc)

        def one(e):
            cols = cols_of(e)
            da = dot_t(dy[rows, :], w2[cols, :])
            lanes = lax.broadcasted_iota(jnp.int32, (count, LANES), 1)
            gate = gate_of(rows, count, e)
            on = gate >= 0.0
            h1 = d1[rows, cols].astype(F32)
            h3 = d3[rows, cols].astype(F32)
            sig = sg[rows, cols]
            silu = h1 * sig
            act = (silu * h3).astype(BF16).astype(F32)
            dgate = jnp.sum(act * da, axis=1, keepdims=True)
            dgacc[0:count, :] = jnp.where(lanes == ep * GROUP + e, dgate, dgacc[0:count, :])
            da = (gate * da).astype(BF16).astype(F32)
            d1[rows, cols] = jnp.where(on, da * (h3 * (sig * (1.0 + h1 * (1.0 - sig)))), 0.0).astype(BF16)
            d3[rows, cols] = jnp.where(on, da * silu, 0.0).astype(BF16)

        over_experts(lo, hi, one)

    outs = []

    def write_out(row, count, pairs, sem):
        rows = pl.ds(row, count)
        copies = [pltpu.make_async_copy(s.at[rows, :], d.at[rows, :], out_sem.at[sem, k]) for k, (s, d) in enumerate(pairs)]
        start(copies)
        outs.extend(copies)

    grads = ((ga, ga_out), (d1, d1_out), (d3, d3_out), (u, u_out), (dy, dy_out))

    def small(i, src, dst, dev):
        return pltpu.make_async_remote_copy(src, dst, small_send.at[i], small_recv.at[i], device_id=dev, device_id_type=MESH)

    dg_copies = {(chip, o): small(2 * chip + o, dgb.at[2 * chip + o], dgr.at[2 * chip + o], device_of(chip, o)) for chip, o in others}
    dl_copies = {(chip, o): small(8 + 2 * chip + o, dlb.at[0], dlb.at[2 * chip + o], device_of(chip, o)) for chip, o in others}

    def send_gates(chips):
        for i, chip in enumerate(chips):
            for o in (0, 1):
                k = 2 * i + o
                dgb[2 * chip + o] = dgacc[k * tok : (k + 1) * tok, :]
                if (chip, o) != (OWN, 0):
                    dg_copies[(chip, o)].start()

    def sums_pass(row, chips, k, lo, hi):
        rows = pl.ds(row, 2 * tok * len(chips))
        width = 256
        for n in range(lo, hi):
            cols = pl.ds(n * width, width)
            tile = dot(ga[rows, :], w2[:, cols]) if k == 0 else dot_t(d1[rows, :], w1[cols, :]) + dot_t(d3[rows, :], w3[cols, :])
            for i, chip in enumerate(chips):
                at = 2 * tok * i
                ys[chip, k, :, cols] = tile[at : at + tok]
                yo[chip, k, :, cols] = tile[at + tok : at + 2 * tok].astype(BF16)

    pair = {
        (first, k): pltpu.make_async_remote_copy(
            yo.at[pl.ds(first, 2), k], yr.at[pl.ds(first, 2), k], pair_send.at[first + k], pair_recv.at[first + k], device_id=partner, device_id_type=MESH
        )
        for first in (OWN, XN)
        for k in (0, 1)
    }
    xy = {
        (chip, k): pltpu.make_async_remote_copy(
            xs.at[chip - XN, k], xr.at[chip - XN, k], xy_send.at[chip - XN, k], xy_recv.at[chip - XN, k], device_id=device_of(chip, 0), device_id_type=MESH
        )
        for chip in (XN, YN)
        for k in (0, 1)
    }

    def send_xy(k):
        pair[(XN, k)].wait_recv()
        for chip in (XN, YN):
            xs[chip - XN, k] = (ys[chip, k] + yr[chip, k].astype(F32)).astype(BF16)
            xy[(chip, k)].start()

    steps = d_model // 256

    wait_recv(to_partner[:2])
    u_pass(0, 2 * tok, 0, unroll, first=True)
    start_w(0, local_exp, slice(2, 3))
    u_pass(0, 2 * tok, unroll, local_exp, first=True)
    to_chip[XN][2].start()
    to_chip[YN][2].start()
    pass_on((0, 1))
    for e in range(local_exp):
        load_w(e)[2].wait()
    sums_pass(0, (OWN,), 0, 0, steps)

    for chip in (XN, YN):
        wait_recv(forward[chip][:2])
    u_pass(4 * tok, 4 * tok, 0, local_exp)
    pass_on((2,))
    sums_pass(4 * tok, (XN, YN), 0, 0, steps)
    pair[(XN, 0)].start()
    for chip in (XN, YN):
        forward[chip][2].wait_recv()
    dy_pass(4 * tok, 4 * tok, 0, unroll)
    for k in range(3):
        for copies in relay.values():
            copies[k].wait_recv()
        forward[DIAG][k].start()
    send_xy(0)
    dy_pass(4 * tok, 4 * tok, unroll, local_exp)
    write_out(4 * tok, 4 * tok, grads, 0)
    send_gates((XN, YN))

    wait_recv(forward[DIAG])
    u_pass(2 * tok, 2 * tok, 0, local_exp)
    to_partner[2].wait_recv()
    dy_pass(0, 4 * tok, 0, local_exp)
    write_out(0, 4 * tok, grads, 1)
    send_gates((OWN, DIAG))

    sums_pass(4 * tok, (XN, YN), 1, 0, steps)
    pair[(XN, 1)].start()

    for c in dg_copies.values():
        c.wait_recv()
    dgate = dgb[0]
    for chip, o in others:
        dgate = dgate + dgr[2 * chip + o]
    own_rt = rt[0:tok, :]
    left = lane < 64
    prob = jnp.where(left, own_rt, 0.0)
    dprob = jnp.where(left & (pltpu.roll(own_rt, 64, 1) >= 0.0), dgate, 0.0)
    dlogit = prob * (dprob - jnp.sum(prob * dprob, axis=1, keepdims=True))
    high = dlogit.astype(BF16)
    low = dlogit - high.astype(F32)
    dlb[0] = jnp.where(left, high.astype(F32), pltpu.roll(low, 64, 1)).astype(BF16)
    start(dl_copies.values())

    sums_pass(2 * tok, (DIAG,), 0, 0, steps)
    pair[(OWN, 0)].start()
    send_xy(1)
    sums_pass(0, (OWN, DIAG), 1, 0, steps)
    pair[(OWN, 1)].start()
    du_router = dot(dlb[0], wr16[...])
    wait_recv(dl_copies.values())
    dl_out[...] = dlb[...].reshape(8 * tok, LANES)
    for k, base in enumerate((u[0:tok, :].astype(F32), dy[0:tok, :].astype(F32) + du_router)):
        pair[(OWN, k)].wait_recv()
        send_out[k] = (ys[DIAG, k] + yr[DIAG, k].astype(F32)).astype(BF16)
        own = ys[OWN, k] + yr[OWN, k].astype(F32) + base
        for chip in (XN, YN):
            xy[(chip, k)].wait_recv()
            own = own + xr[chip - XN, k].astype(F32)
        own_out[k] = own

    for copies in (to_partner, *to_chip.values(), *forward.values(), *relay.values(), dg_copies.values(), dl_copies.values(), pair.values(), xy.values()):
        for c in copies:
            c.wait_send()
    for c in outs:
        c.wait()


def grads_kernel(local_exp, u_ref, dy_ref, ga_ref, d1_ref, d3_ref, dl_ref, dwg_ref, dwu_ref, dwd_ref, dwr_ref, xt):
    def over_tokens(a, b):
        return lax.dot_general(a, b, (((0,), (0,)), ((), ())), preferred_element_type=F32)

    @pl.when(pl.program_id(0) == 0)
    def _():
        xt[...] = u_ref[...].T
        wide = over_tokens(dl_ref[...], u_ref[...])
        wide = wide[0:64] + wide[64:128]
        for g in range(dwr_ref.shape[0] // local_exp):
            dwr_ref[g * local_exp : (g + 1) * local_exp, :] = wide[g * GROUP : g * GROUP + local_exp]

    dwg_ref[0] = dot(xt[...], d1_ref[...])
    dwu_ref[0] = dot(xt[...], d3_ref[...])
    dwd_ref[0] = over_tokens(ga_ref[...], dy_ref[...])


def solution(mesh):
    tok_spec = P(("dp", "ep", "etp"), None)
    col_spec = P("ep", None, "etp")
    row_spec = P("ep", "etp", None)
    in_specs = (tok_spec, tok_spec, tok_spec, P(None, None), col_spec, col_spec, row_spec)
    out_specs = (tok_spec, tok_spec, P(("dp", "ep"), None, "etp"), P(("dp", "ep"), None, "etp"), P(("dp", "ep"), "etp", None), P("dp", None))

    def device_step(u_loc, dy_loc, ids_loc, w_router, w_gate, w_up, w_down):
        tok, d_model = u_loc.shape
        top_k = ids_loc.shape[1]
        experts = w_router.shape[1]
        local_exp, _, ffn = w_gate.shape
        rows = 8 * tok
        wide = local_exp * ffn
        any_spec = pl.BlockSpec(memory_space=pl.ANY)
        vmem_spec = pl.BlockSpec(memory_space=pltpu.VMEM)
        S = jax.ShapeDtypeStruct
        dma = pltpu.SemaphoreType.DMA
        u, dy, ga, d1, d3, dl, own, send = pl.pallas_call(
            functools.partial(rows_kernel, (tok, d_model, ffn, local_exp, experts, top_k)),
            name="expert_rows",
            in_specs=[any_spec, any_spec, vmem_spec, vmem_spec, any_spec, any_spec, any_spec],
            out_specs=[any_spec] * 5 + [vmem_spec] * 3,
            out_shape=[
                S((rows, d_model), BF16), S((rows, d_model), BF16),
                S((rows, wide), BF16), S((rows, wide), BF16), S((rows, wide), BF16),
                S((rows, LANES), BF16), S((2, tok, d_model), F32), S((2, tok, d_model), BF16),
            ],
            scratch_shapes=[
                pltpu.VMEM((rows, d_model), BF16), pltpu.VMEM((rows, d_model), BF16),
                pltpu.VMEM((rows, LANES), F32),
                pltpu.VMEM((d_model, wide), BF16), pltpu.VMEM((d_model, wide), BF16), pltpu.VMEM((wide, d_model), BF16),
                pltpu.VMEM((rows, wide), BF16), pltpu.VMEM((rows, wide), BF16), pltpu.VMEM((rows, wide), BF16), pltpu.VMEM((rows, wide), F32),
                pltpu.VMEM((4, 2, tok, d_model), F32),
                pltpu.VMEM((4, 2, tok, d_model), BF16), pltpu.VMEM((4, 2, tok, d_model), BF16),
                pltpu.VMEM((2, 2, tok, d_model), BF16), pltpu.VMEM((2, 2, tok, d_model), BF16),
                pltpu.VMEM((4 * tok, LANES), F32),
                pltpu.VMEM((8, tok, LANES), F32), pltpu.VMEM((8, tok, LANES), F32),
                pltpu.VMEM((8, tok, LANES), BF16),
                pltpu.VMEM((LANES, d_model), BF16),
                dma((2,)), dma((3, local_exp)), dma((3, 8)), dma((3, 8)), dma((16,)), dma((16,)),
                dma((4,)), dma((4,)), dma((2, 2)), dma((2, 2)), dma((2, 5)),
            ],
            compiler_params=pltpu.CompilerParams(collective_id=0, has_side_effects=True, vmem_limit_bytes=62 * 1024 * 1024),
        )(u_loc, dy_loc, ids_loc.T, w_router.T, w_gate, w_up, w_down)

        n_ep, n_etp = lax.axis_size("ep"), lax.axis_size("etp")
        got = lax.ppermute(send, ("etp", "ep"), [(i, i ^ (n_ep + 2)) for i in range(n_ep * n_etp)])

        col_block = pl.BlockSpec((rows, ffn), lambda e: (0, e))
        whole_rows = pl.BlockSpec((rows, d_model), lambda e: (0, 0))
        dwg, dwu, dwd, dwr = pl.pallas_call(
            functools.partial(grads_kernel, local_exp),
            name="weight_grads",
            grid=(local_exp,),
            in_specs=[whole_rows, whole_rows, col_block, col_block, col_block, pl.BlockSpec((rows, LANES), lambda e: (0, 0))],
            out_specs=[
                pl.BlockSpec((1, d_model, ffn), lambda e: (e, 0, 0)),
                pl.BlockSpec((1, d_model, ffn), lambda e: (e, 0, 0)),
                pl.BlockSpec((1, ffn, d_model), lambda e: (e, 0, 0)),
                pl.BlockSpec((experts, d_model), lambda e: (0, 0)),
            ],
            out_shape=[S((local_exp, d_model, ffn), F32), S((local_exp, d_model, ffn), F32), S((local_exp, ffn, d_model), F32), S((experts, d_model), F32)],
            scratch_shapes=[pltpu.VMEM((d_model, rows), BF16)],
            compiler_params=pltpu.CompilerParams(vmem_limit_bytes=62 * 1024 * 1024),
            cost_estimate=pl.CostEstimate(flops=3 * 2 * rows * wide * d_model, bytes_accessed=12 * wide * d_model + 10 * rows * wide, transcendentals=0),
        )(u, dy, ga, d1, d3, dl)

        y_loc = (own[0] + got[0].astype(F32)).astype(BF16)
        du_loc = (own[1] + got[1].astype(F32)).astype(BF16)
        return y_loc, du_loc, dwg, dwu, dwd, dwr.T

    return jax.shard_map(device_step, mesh=mesh, in_specs=in_specs, out_specs=out_specs, check_vma=False)
```

```python
import functools

import jax
import jax.numpy as jnp
from jax import lax
from jax.experimental import pallas as pl
from jax.experimental.pallas import tpu as pltpu
from jax.sharding import PartitionSpec as P

MESH = pl.DeviceIdType.MESH
F32 = jnp.float32
BF16 = jnp.bfloat16
LANES = 128
GROUP = 16
OWN, DIAG, XN, YN = 0, 1, 2, 3


def dot(a, b):
    return jnp.dot(a, b, preferred_element_type=F32)


def dot_t(a, b):
    return lax.dot_general(a, b, (((1,), (1,)), ((), ())), preferred_element_type=F32)


def flip(index, bit):
    return index + bit - 2 * index * bit


def device_of(chip, other):
    ep, etp = lax.axis_index("ep"), lax.axis_index("etp")
    xb, yb = {OWN: (0, 0), DIAG: (1, 1), XN: (1, 0), YN: (0, 1)}[chip]
    return {"dp": lax.axis_index("dp"), "etp": flip(etp, yb), "ep": flip(ep // 2, xb) * 2 + flip(ep % 2, other)}


def rows_kernel(
    sizes, u_hbm, dy_hbm, ids_ref, wr_ref, wg_hbm, wu_hbm, wd_hbm,
    dy, ga, d1, d3, xt, dl_out, own_out, send_out,
    u, rt, w1, w3, w2, sg, ys, yo, yr, xs, xr, dgacc, dgb, dgr, dlb, wr16,
    in_sem, w_sem, ag_send, ag_recv, small_send, small_recv, pair_send, pair_recv, xy_send, xy_recv,
):
    tok, d_model, ffn, local_exp, experts, top_k = sizes
    ep = lax.axis_index("ep")

    load_rows = [pltpu.make_async_copy(src, dst.at[pl.ds(0, tok), :], in_sem.at[k]) for k, (src, dst) in enumerate(((u_hbm, u), (dy_hbm, dy)))]
    for c in load_rows:
        c.start()

    def load_w(e):
        cols = pl.ds(pl.multiple_of(e * ffn, ffn), ffn)
        return [
            pltpu.make_async_copy(wg_hbm.at[e], w1.at[:, cols], w_sem.at[0, e]),
            pltpu.make_async_copy(wu_hbm.at[e], w3.at[:, cols], w_sem.at[1, e]),
            pltpu.make_async_copy(wd_hbm.at[e], w2.at[cols, :], w_sem.at[2, e]),
        ]

    barrier = pltpu.get_barrier_semaphore()
    others = [(chip, o) for chip in (OWN, DIAG, XN, YN) for o in (0, 1) if (chip, o) != (OWN, 0)]
    for chip, o in others:
        pl.semaphore_signal(barrier, inc=1, device_id=device_of(chip, o), device_id_type=MESH)

    slot40 = lax.broadcasted_iota(jnp.int32, (LANES, experts), 0) % 64
    col40 = lax.broadcasted_iota(jnp.int32, (LANES, experts), 1)
    spread = (col40 == (slot40 // GROUP) * local_exp + slot40 % GROUP) & (slot40 % GROUP < local_exp)
    wr16[...] = dot(jnp.where(spread, 1.0, 0.0).astype(BF16), wr_ref[...]).astype(BF16)
    slot_t = lax.broadcasted_iota(jnp.int32, (LANES, tok), 0) % 64
    expert_t = jnp.where(slot_t % GROUP < local_exp, (slot_t // GROUP) * local_exp + slot_t % GROUP, -1)
    chosen_t = jnp.zeros((LANES, tok), F32)
    for j in range(top_k):
        chosen_t = jnp.where(expert_t == ids_ref[j : j + 1, :], 1.0, chosen_t)
    chosen = chosen_t.T > 0.5
    lane = lax.broadcasted_iota(jnp.int32, (tok, LANES), 1)
    valid = lane % GROUP < local_exp
    for c in load_rows:
        c.wait()
    unroll = 5

    def start_w(lo, hi, which):
        for e in range(lo, hi):
            for c in load_w(e)[which]:
                c.start()

    start_w(0, unroll, slice(0, 2))

    logits = jnp.where(valid, dot_t(u[0:tok, :], wr16[...]), -1e30)
    top = jnp.max(logits, axis=1, keepdims=True)
    expo = jnp.where(valid, jnp.exp(logits - top), 0.0)
    prob = expo / jnp.sum(jnp.where(lane < 64, expo, 0.0), axis=1, keepdims=True)
    rt[0:tok, :] = jnp.where((lane < 64) | chosen, prob, -1.0)

    pl.semaphore_wait(barrier, len(others))
    start_w(unroll, local_exp, slice(0, 2))

    def block(chip, o):
        return pl.ds((2 * chip + o) * tok, tok)

    def gather(i, src, dst, dev):
        return [
            pltpu.make_async_remote_copy(ref.at[src, :], ref.at[dst, :], ag_send.at[k, i], ag_recv.at[k, i], device_id=dev, device_id_type=MESH)
            for k, ref in enumerate((rt, u, dy))
        ]

    partner = device_of(OWN, 1)
    to_partner = gather(0, block(OWN, 0), block(OWN, 1), partner)
    to_chip = {chip: gather(chip, block(OWN, 0), block(chip, 0), device_of(chip, 0)) for chip in (XN, YN)}
    forward = {chip: gather(3 + chip, block(chip, 0), block(chip, 1), partner) for chip in (DIAG, XN, YN)}
    half = tok // 2

    def half_of(chip, h):
        return pl.ds(2 * chip * tok + h * half, half)

    relay = {
        YN: gather(1, half_of(YN, 1), half_of(DIAG, 1), device_of(XN, 0)),
        XN: gather(7, half_of(XN, 0), half_of(DIAG, 0), device_of(YN, 0)),
    }

    def start(copies):
        for c in copies:
            c.start()

    def wait_recv(copies):
        for c in copies:
            c.wait_recv()

    for k in range(2):
        for copies in (to_partner, to_chip[XN], to_chip[YN]):
            copies[k].start()
    to_partner[2].start()

    def pass_on(parts):
        for chip in (XN, YN):
            for k in parts:
                to_chip[chip][k].wait_recv()
                relay[chip][k].start()
                forward[chip][k].start()

    def cols_of(e):
        return pl.ds(pl.multiple_of(e * ffn, ffn), ffn)

    def gate_of(rows, count, e):
        lanes = lax.broadcasted_iota(jnp.int32, (count, LANES), 1)
        return jnp.sum(jnp.where(lanes == 64 + ep * GROUP + e, rt[rows, :], 0.0), axis=1, keepdims=True)

    def over_experts(lo, hi, one, which=None):
        def body(i, carry):
            if which is not None:
                for k in range(unroll):
                    for c in load_w(i * unroll + k)[which]:
                        c.wait()
            for k in range(unroll):
                one(i * unroll + k)
            return carry

        lax.fori_loop(lo // unroll, hi // unroll, body, 0)

    def u_pass(row, count, lo, hi, first=False):
        rows = pl.ds(row, count)

        def one(e):
            cols = cols_of(e)
            h1 = dot(u[rows, :], w1[:, cols]).astype(BF16)
            h3 = dot(u[rows, :], w3[:, cols]).astype(BF16)
            d1[rows, cols] = h1
            d3[rows, cols] = h3
            gate = gate_of(rows, count, e)
            h1 = h1.astype(F32)
            sig = jax.nn.sigmoid(h1)
            sg[rows, cols] = sig
            act = (h1 * sig * h3.astype(F32)).astype(BF16).astype(F32)
            ga[rows, cols] = jnp.where(gate >= 0.0, gate * act, 0.0).astype(BF16)

        over_experts(lo, hi, one, slice(0, 2) if first else None)

    def dy_pass(row, count, lo, hi):
        rows = pl.ds(row, count)
        if lo == 0:
            dgacc[...] = jnp.zeros_like(dgacc)

        def one(e):
            cols = cols_of(e)
            da = dot_t(dy[rows, :], w2[cols, :])
            lanes = lax.broadcasted_iota(jnp.int32, (count, LANES), 1)
            gate = gate_of(rows, count, e)
            on = gate >= 0.0
            h1 = d1[rows, cols].astype(F32)
            h3 = d3[rows, cols].astype(F32)
            sig = sg[rows, cols]
            silu = h1 * sig
            act = (silu * h3).astype(BF16).astype(F32)
            dgate = jnp.sum(act * da, axis=1, keepdims=True)
            dgacc[0:count, :] = jnp.where(lanes == ep * GROUP + e, dgate, dgacc[0:count, :])
            da = (gate * da).astype(BF16).astype(F32)
            d1[rows, cols] = jnp.where(on, da * (h3 * (sig * (1.0 + h1 * (1.0 - sig)))), 0.0).astype(BF16)
            d3[rows, cols] = jnp.where(on, da * silu, 0.0).astype(BF16)

        over_experts(lo, hi, one)

    def small(i, src, dst, dev):
        return pltpu.make_async_remote_copy(src, dst, small_send.at[i], small_recv.at[i], device_id=dev, device_id_type=MESH)

    dg_copies = {(chip, o): small(2 * chip + o, dgb.at[2 * chip + o], dgr.at[2 * chip + o], device_of(chip, o)) for chip, o in others}
    dl_copies = {(chip, o): small(8 + 2 * chip + o, dlb.at[0], dlb.at[2 * chip + o], device_of(chip, o)) for chip, o in others}

    def send_gates(chips):
        for i, chip in enumerate(chips):
            for o in (0, 1):
                k = 2 * i + o
                dgb[2 * chip + o] = dgacc[k * tok : (k + 1) * tok, :]
                if (chip, o) != (OWN, 0):
                    dg_copies[(chip, o)].start()

    def sums_pass(row, chips, k, lo, hi, transpose=False):
        rows = pl.ds(row, 2 * tok * len(chips))
        width = 256
        for n in range(lo, hi):
            cols = pl.ds(n * width, width)
            tile = dot(ga[rows, :], w2[:, cols]) if k == 0 else dot_t(d1[rows, :], w1[cols, :]) + dot_t(d3[rows, :], w3[cols, :])
            if transpose:
                xt[cols, :] = u[:, cols].T
            for i, chip in enumerate(chips):
                at = 2 * tok * i
                ys[chip, k, :, cols] = tile[at : at + tok]
                yo[chip, k, :, cols] = tile[at + tok : at + 2 * tok].astype(BF16)

    pair = {
        (first, k): pltpu.make_async_remote_copy(
            yo.at[pl.ds(first, 2), k], yr.at[pl.ds(first, 2), k], pair_send.at[first + k], pair_recv.at[first + k], device_id=partner, device_id_type=MESH
        )
        for first in (OWN, XN)
        for k in (0, 1)
    }
    xy = {
        (chip, k): pltpu.make_async_remote_copy(
            xs.at[chip - XN, k], xr.at[chip - XN, k], xy_send.at[chip - XN, k], xy_recv.at[chip - XN, k], device_id=device_of(chip, 0), device_id_type=MESH
        )
        for chip in (XN, YN)
        for k in (0, 1)
    }

    def send_xy(k):
        pair[(XN, k)].wait_recv()
        for chip in (XN, YN):
            xs[chip - XN, k] = (ys[chip, k] + yr[chip, k].astype(F32)).astype(BF16)
            xy[(chip, k)].start()

    steps = d_model // 256

    wait_recv(to_partner[:2])
    u_pass(0, 2 * tok, 0, unroll, first=True)
    start_w(0, local_exp, slice(2, 3))
    u_pass(0, 2 * tok, unroll, local_exp, first=True)
    to_chip[XN][2].start()
    to_chip[YN][2].start()
    pass_on((0, 1))
    for e in range(local_exp):
        load_w(e)[2].wait()
    sums_pass(0, (OWN,), 0, 0, steps)

    for chip in (XN, YN):
        wait_recv(forward[chip][:2])
    u_pass(4 * tok, 4 * tok, 0, local_exp)
    pass_on((2,))
    sums_pass(4 * tok, (XN, YN), 0, 0, steps)
    pair[(XN, 0)].start()
    for chip in (XN, YN):
        forward[chip][2].wait_recv()
    dy_pass(4 * tok, 4 * tok, 0, unroll)
    for k in range(3):
        for copies in relay.values():
            copies[k].wait_recv()
        forward[DIAG][k].start()
    send_xy(0)
    dy_pass(4 * tok, 4 * tok, unroll, local_exp)
    send_gates((XN, YN))

    wait_recv(forward[DIAG])
    u_pass(2 * tok, 2 * tok, 0, local_exp)
    to_partner[2].wait_recv()
    dy_pass(0, 4 * tok, 0, local_exp)
    send_gates((OWN, DIAG))

    sums_pass(4 * tok, (XN, YN), 1, 0, steps, transpose=True)
    pair[(XN, 1)].start()

    for c in dg_copies.values():
        c.wait_recv()
    dgate = dgb[0]
    for chip, o in others:
        dgate = dgate + dgr[2 * chip + o]
    own_rt = rt[0:tok, :]
    left = lane < 64
    prob = jnp.where(left, own_rt, 0.0)
    dprob = jnp.where(left & (pltpu.roll(own_rt, 64, 1) >= 0.0), dgate, 0.0)
    dlogit = prob * (dprob - jnp.sum(prob * dprob, axis=1, keepdims=True))
    high = dlogit.astype(BF16)
    low = dlogit - high.astype(F32)
    dlb[0] = jnp.where(left, high.astype(F32), pltpu.roll(low, 64, 1)).astype(BF16)
    start(dl_copies.values())

    sums_pass(2 * tok, (DIAG,), 0, 0, steps)
    pair[(OWN, 0)].start()
    send_xy(1)
    sums_pass(0, (OWN, DIAG), 1, 0, steps)
    pair[(OWN, 1)].start()
    du_router = dot(dlb[0], wr16[...])
    wait_recv(dl_copies.values())
    dl_out[...] = dlb[...].reshape(8 * tok, LANES)
    for k, base in enumerate((u[0:tok, :].astype(F32), dy[0:tok, :].astype(F32) + du_router)):
        pair[(OWN, k)].wait_recv()
        send_out[k] = (ys[DIAG, k] + yr[DIAG, k].astype(F32)).astype(BF16)
        own = ys[OWN, k] + yr[OWN, k].astype(F32) + base
        for chip in (XN, YN):
            xy[(chip, k)].wait_recv()
            own = own + xr[chip - XN, k].astype(F32)
        own_out[k] = own

    for copies in (to_partner, *to_chip.values(), *forward.values(), *relay.values(), dg_copies.values(), dl_copies.values(), pair.values(), xy.values()):
        for c in copies:
            c.wait_send()


def grads_kernel(sizes, xt, dy, ga, d1, d3, dl, dwg_hbm, dwu_hbm, dwd_hbm, dwr_ref, gu, dn, sems):
    local_exp, ffn = sizes

    def copies(e, slot):
        return [
            pltpu.make_async_copy(gu.at[slot, :, pl.ds(0, ffn)], dwg_hbm.at[e], sems.at[0, slot]),
            pltpu.make_async_copy(gu.at[slot, :, pl.ds(ffn, ffn)], dwu_hbm.at[e], sems.at[1, slot]),
            pltpu.make_async_copy(dn.at[slot], dwd_hbm.at[e], sems.at[2, slot]),
        ]

    def one(e, slot):
        cols = pl.ds(pl.multiple_of(e * ffn, ffn), ffn)
        gu[slot] = dot(xt[...], jnp.concatenate([d1[:, cols], d3[:, cols]], axis=1))
        for c in copies(e, slot)[:2]:
            c.start()
        dn[slot] = lax.dot_general(ga[:, cols], dy[...], (((0,), (0,)), ((), ())), preferred_element_type=F32)
        copies(e, slot)[2].start()

    def body(i, carry):
        for slot in (0, 1):

            @pl.when(i > 0)
            def _():
                for c in copies(2 * i + slot - 2, slot):
                    c.wait()

            one(2 * i + slot, slot)
        return carry

    lax.fori_loop(0, local_exp // 2, body, 0)
    wide = dot_t(dl[...].T, xt[...])
    wide = wide[0:64] + wide[64:128]
    for g in range(dwr_ref.shape[0] // local_exp):
        dwr_ref[g * local_exp : (g + 1) * local_exp, :] = wide[g * GROUP : g * GROUP + local_exp]
    for slot in (0, 1):
        for c in copies(local_exp - 2 + slot, slot):
            c.wait()


def solution(mesh):
    tok_spec = P(("dp", "ep", "etp"), None)
    col_spec = P("ep", None, "etp")
    row_spec = P("ep", "etp", None)
    in_specs = (tok_spec, tok_spec, tok_spec, P(None, None), col_spec, col_spec, row_spec)
    out_specs = (tok_spec, tok_spec, P(("dp", "ep"), None, "etp"), P(("dp", "ep"), None, "etp"), P(("dp", "ep"), "etp", None), P("dp", None))

    def device_step(u_loc, dy_loc, ids_loc, w_router, w_gate, w_up, w_down):
        tok, d_model = u_loc.shape
        top_k = ids_loc.shape[1]
        experts = w_router.shape[1]
        local_exp, _, ffn = w_gate.shape
        rows = 8 * tok
        wide = local_exp * ffn
        any_spec = pl.BlockSpec(memory_space=pl.ANY)
        vmem_spec = pl.BlockSpec(memory_space=pltpu.VMEM)
        S = jax.ShapeDtypeStruct
        dma = pltpu.SemaphoreType.DMA
        dy, ga, d1, d3, xt, dl, own, send = pl.pallas_call(
            functools.partial(rows_kernel, (tok, d_model, ffn, local_exp, experts, top_k)),
            name="expert_rows",
            in_specs=[any_spec, any_spec, vmem_spec, vmem_spec, any_spec, any_spec, any_spec],
            out_specs=[vmem_spec] * 8,
            out_shape=[
                pltpu.VMEM((rows, d_model), BF16),
                pltpu.VMEM((rows, wide), BF16), pltpu.VMEM((rows, wide), BF16), pltpu.VMEM((rows, wide), BF16),
                pltpu.VMEM((d_model, rows), BF16), pltpu.VMEM((rows, LANES), BF16),
                S((2, tok, d_model), F32), S((2, tok, d_model), BF16),
            ],
            scratch_shapes=[
                pltpu.VMEM((rows, d_model), BF16),
                pltpu.VMEM((rows, LANES), F32),
                pltpu.VMEM((d_model, wide), BF16), pltpu.VMEM((d_model, wide), BF16), pltpu.VMEM((wide, d_model), BF16),
                pltpu.VMEM((rows, wide), F32),
                pltpu.VMEM((4, 2, tok, d_model), F32),
                pltpu.VMEM((4, 2, tok, d_model), BF16), pltpu.VMEM((4, 2, tok, d_model), BF16),
                pltpu.VMEM((2, 2, tok, d_model), BF16), pltpu.VMEM((2, 2, tok, d_model), BF16),
                pltpu.VMEM((4 * tok, LANES), F32),
                pltpu.VMEM((8, tok, LANES), F32), pltpu.VMEM((8, tok, LANES), F32),
                pltpu.VMEM((8, tok, LANES), BF16),
                pltpu.VMEM((LANES, d_model), BF16),
                dma((2,)), dma((3, local_exp)), dma((3, 8)), dma((3, 8)), dma((16,)), dma((16,)),
                dma((4,)), dma((4,)), dma((2, 2)), dma((2, 2)),
            ],
            compiler_params=pltpu.CompilerParams(collective_id=0, has_side_effects=True, vmem_limit_bytes=48 * 1024 * 1024),
        )(u_loc, dy_loc, ids_loc.T, w_router.T, w_gate, w_up, w_down)

        n_ep, n_etp = lax.axis_size("ep"), lax.axis_size("etp")
        got = lax.ppermute(send, ("etp", "ep"), [(i, i ^ (n_ep + 2)) for i in range(n_ep * n_etp)])

        kept = [pltpu.with_memory_space_constraint(a, pltpu.VMEM) for a in (xt, dy, ga, d1, d3, dl)]
        dwg, dwu, dwd, dwr = pl.pallas_call(
            functools.partial(grads_kernel, (local_exp, ffn)),
            name="weight_grads",
            in_specs=[vmem_spec] * 6,
            out_specs=[any_spec] * 3 + [vmem_spec],
            out_shape=[S((local_exp, d_model, ffn), F32), S((local_exp, d_model, ffn), F32), S((local_exp, ffn, d_model), F32), S((experts, d_model), F32)],
            scratch_shapes=[pltpu.VMEM((2, d_model, 2 * ffn), F32), pltpu.VMEM((2, ffn, d_model), F32), dma((3, 2))],
            compiler_params=pltpu.CompilerParams(vmem_limit_bytes=24 * 1024 * 1024),
            cost_estimate=pl.CostEstimate(flops=3 * 2 * rows * wide * d_model, bytes_accessed=12 * wide * d_model + 10 * rows * wide, transcendentals=0),
        )(*kept)

        y_loc = (own[0] + got[0].astype(F32)).astype(BF16)
        du_loc = (own[1] + got[1].astype(F32)).astype(BF16)
        return y_loc, du_loc, dwg, dwu, dwd, dwr.T

    return jax.shard_map(device_step, mesh=mesh, in_specs=in_specs, out_specs=out_specs, check_vma=False)
```

```python
import functools

import jax
import jax.numpy as jnp
from jax import lax
from jax.experimental import pallas as pl
from jax.experimental.pallas import tpu as pltpu
from jax.sharding import PartitionSpec as P

MESH = pl.DeviceIdType.MESH
F32 = jnp.float32
BF16 = jnp.bfloat16
LANES = 128
GROUP = 16
OWN, DIAG, XN, YN = 0, 1, 2, 3


def dot(a, b):
    return jnp.dot(a, b, preferred_element_type=F32)


def dot_t(a, b):
    return lax.dot_general(a, b, (((1,), (1,)), ((), ())), preferred_element_type=F32)


def flip(index, bit):
    return index + bit - 2 * index * bit


def device_of(chip, other):
    ep, etp = lax.axis_index("ep"), lax.axis_index("etp")
    xb, yb = {OWN: (0, 0), DIAG: (1, 1), XN: (1, 0), YN: (0, 1)}[chip]
    return {"dp": lax.axis_index("dp"), "etp": flip(etp, yb), "ep": flip(ep // 2, xb) * 2 + flip(ep % 2, other)}


def rows_kernel(
    sizes, u_hbm, dy_hbm, ids_hbm, wr_hbm, wg_hbm, wu_hbm, wd_hbm,
    dy, ga, d1, d3, xt, dl_out, own_out, send_out,
    u, ids_ref, wr_ref, rt, w1, w3, w2, sg, das, ys, yo, yr, xs, xr, dgacc, dgb, dgr, dlb, wr16,
    in_sem, w_sem, ag_send, ag_recv, small_send, small_recv, pair_send, pair_recv, xy_send, xy_recv,
):
    tok, d_model, ffn, local_exp, experts, top_k = sizes
    ep = lax.axis_index("ep")

    load_rows = [pltpu.make_async_copy(src, dst.at[pl.ds(0, tok), :], in_sem.at[k]) for k, (src, dst) in enumerate(((u_hbm, u), (dy_hbm, dy)))]
    load_small = [pltpu.make_async_copy(src, dst, in_sem.at[2 + k]) for k, (src, dst) in enumerate(((wr_hbm, wr_ref), (ids_hbm, ids_ref)))]
    for c in load_rows + load_small:
        c.start()

    def load_w(e):
        cols = pl.ds(pl.multiple_of(e * ffn, ffn), ffn)
        return [
            pltpu.make_async_copy(wg_hbm.at[e], w1.at[:, cols], w_sem.at[0, e]),
            pltpu.make_async_copy(wu_hbm.at[e], w3.at[:, cols], w_sem.at[1, e]),
            pltpu.make_async_copy(wd_hbm.at[e], w2.at[cols, :], w_sem.at[2, e]),
        ]

    unroll = 5

    def start_w(lo, hi, which):
        for e in range(lo, hi):
            for c in load_w(e)[which]:
                c.start()

    start_w(0, 1, slice(0, 2))

    barrier = pltpu.get_barrier_semaphore()
    others = [(chip, o) for chip in (OWN, DIAG, XN, YN) for o in (0, 1) if (chip, o) != (OWN, 0)]
    for chip, o in others:
        pl.semaphore_signal(barrier, inc=1, device_id=device_of(chip, o), device_id_type=MESH)

    def block(chip, o):
        return pl.ds((2 * chip + o) * tok, tok)

    def gather(i, src, dst, dev):
        return [
            pltpu.make_async_remote_copy(ref.at[src, :], ref.at[dst, :], ag_send.at[k, i], ag_recv.at[k, i], device_id=dev, device_id_type=MESH)
            for k, ref in enumerate((rt, u, dy))
        ]

    partner = device_of(OWN, 1)
    to_partner = gather(0, block(OWN, 0), block(OWN, 1), partner)
    to_chip = {chip: gather(chip, block(OWN, 0), block(chip, 0), device_of(chip, 0)) for chip in (XN, YN)}
    forward = {chip: gather(3 + chip, block(chip, 0), block(chip, 1), partner) for chip in (DIAG, XN, YN)}
    half = tok // 2

    def half_of(chip, h):
        return pl.ds(2 * chip * tok + h * half, half)

    relay = {
        YN: gather(1, half_of(YN, 1), half_of(DIAG, 1), device_of(XN, 0)),
        XN: gather(7, half_of(XN, 0), half_of(DIAG, 0), device_of(YN, 0)),
    }

    def start(copies):
        for c in copies:
            c.start()

    def wait_recv(copies):
        for c in copies:
            c.wait_recv()

    def send_part(k, chips):
        for copies in chips:
            copies[k].start()

    first_chips = (to_partner, to_chip[XN], to_chip[YN])
    for c in load_rows:
        c.wait()
    start_w(1, local_exp, slice(0, 2))
    pl.semaphore_wait(barrier, len(others))
    send_part(1, first_chips)

    slot40 = lax.broadcasted_iota(jnp.int32, (LANES, experts), 0) % 64
    col40 = lax.broadcasted_iota(jnp.int32, (LANES, experts), 1)
    spread = (col40 == (slot40 // GROUP) * local_exp + slot40 % GROUP) & (slot40 % GROUP < local_exp)
    for c in load_small:
        c.wait()
    wr16[...] = dot(jnp.where(spread, 1.0, 0.0).astype(BF16), wr_ref[...]).astype(BF16)
    slot_t = lax.broadcasted_iota(jnp.int32, (LANES, tok), 0) % 64
    expert_t = jnp.where(slot_t % GROUP < local_exp, (slot_t // GROUP) * local_exp + slot_t % GROUP, -1)
    chosen_t = jnp.zeros((LANES, tok), F32)
    for j in range(top_k):
        chosen_t = jnp.where(expert_t == ids_ref[j : j + 1, :], 1.0, chosen_t)
    chosen = chosen_t.T > 0.5
    lane = lax.broadcasted_iota(jnp.int32, (tok, LANES), 1)
    valid = lane % GROUP < local_exp
    logits = jnp.where(valid, dot_t(u[0:tok, :], wr16[...]), -1e30)
    top = jnp.max(logits, axis=1, keepdims=True)
    expo = jnp.where(valid, jnp.exp(logits - top), 0.0)
    prob = expo / jnp.sum(jnp.where(lane < 64, expo, 0.0), axis=1, keepdims=True)
    rt[0:tok, :] = jnp.where((lane < 64) | chosen, prob, -1.0)
    send_part(0, first_chips)
    to_partner[2].start()

    def pass_on(parts):
        for chip in (XN, YN):
            for k in parts:
                to_chip[chip][k].wait_recv()
                relay[chip][k].start()
                forward[chip][k].start()

    def cols_of(e):
        return pl.ds(pl.multiple_of(e * ffn, ffn), ffn)

    def gate_of(rows, count, e):
        lanes = lax.broadcasted_iota(jnp.int32, (count, LANES), 1)
        return jnp.sum(jnp.where(lanes == 64 + ep * GROUP + e, rt[rows, :], 0.0), axis=1, keepdims=True)

    def over_experts(lo, hi, one, which=None):
        def body(i, carry):
            if which is not None:
                for k in range(unroll):
                    for c in load_w(i * unroll + k)[which]:
                        c.wait()
            for k in range(unroll):
                one(i * unroll + k, k % 2)
            return carry

        lax.fori_loop(lo // unroll, hi // unroll, body, 0)

    def u_pass(row, count, lo, hi, first=False):
        rows = pl.ds(row, count)

        def one(e, slot):
            cols = cols_of(e)
            gate = gate_of(rows, count, e)
            on = gate >= 0.0
            h1 = jnp.where(on, dot(u[rows, :], w1[:, cols]), 0.0).astype(BF16)
            h3 = jnp.where(on, dot(u[rows, :], w3[:, cols]), 0.0).astype(BF16)
            d1[rows, cols] = h1
            d3[rows, cols] = h3
            h1 = h1.astype(F32)
            sig = jax.nn.sigmoid(h1)
            sg[rows, cols] = sig
            act = (h1 * sig * h3.astype(F32)).astype(BF16).astype(F32)
            ga[rows, cols] = (gate * act).astype(BF16)

        over_experts(lo, hi, one, slice(0, 2) if first else None)

    def dy_pass(row, count, lo, hi):
        rows = pl.ds(row, count)
        if lo == 0:
            dgacc[...] = jnp.zeros_like(dgacc)

        def one(e, slot):
            cols = cols_of(e)
            das[slot, 0:count, :] = dot_t(dy[rows, :], w2[cols, :])
            for at in range(0, count, tok):
                part = pl.ds(row + at, tok)
                lanes = lax.broadcasted_iota(jnp.int32, (tok, LANES), 1)
                gate = gate_of(part, tok, e)
                h1 = d1[part, cols].astype(F32)
                h3 = d3[part, cols].astype(F32)
                sig = sg[part, cols]
                silu = h1 * sig
                da = das[slot, at : at + tok, :]
                act = (silu * h3).astype(BF16).astype(F32)
                dgate = jnp.sum(act * da, axis=1, keepdims=True)
                dgacc[at : at + tok, :] = jnp.where(lanes == ep * GROUP + e, dgate, dgacc[at : at + tok, :])
                da = jnp.where(gate >= 0.0, gate * da, 0.0).astype(BF16).astype(F32)
                d1[part, cols] = (da * h3 * (sig + silu - silu * sig)).astype(BF16)
                d3[part, cols] = (da * silu).astype(BF16)

        over_experts(lo, hi, one)

    def small(i, src, dst, dev):
        return pltpu.make_async_remote_copy(src, dst, small_send.at[i], small_recv.at[i], device_id=dev, device_id_type=MESH)

    dg_copies = {(chip, o): small(2 * chip + o, dgb.at[2 * chip + o], dgr.at[2 * chip + o], device_of(chip, o)) for chip, o in others}
    dl_copies = {(chip, o): small(8 + 2 * chip + o, dlb.at[0], dlb.at[2 * chip + o], device_of(chip, o)) for chip, o in others}

    def send_gates(chips):
        for i, chip in enumerate(chips):
            for o in (0, 1):
                k = 2 * i + o
                dgb[2 * chip + o] = dgacc[k * tok : (k + 1) * tok, :]
                if (chip, o) != (OWN, 0):
                    dg_copies[(chip, o)].start()

    def sums_pass(row, chips, k, lo, hi, transpose=False):
        rows = pl.ds(row, 2 * tok * len(chips))
        width = 256
        for n in range(lo, hi):
            cols = pl.ds(n * width, width)
            tile = dot(ga[rows, :], w2[:, cols]) if k == 0 else dot_t(d1[rows, :], w1[cols, :]) + dot_t(d3[rows, :], w3[cols, :])
            if transpose:
                xt[cols, :] = u[:, cols].T
            for i, chip in enumerate(chips):
                at = 2 * tok * i
                ys[chip, k, :, cols] = tile[at : at + tok]
                yo[chip, k, :, cols] = tile[at + tok : at + 2 * tok].astype(BF16)

    steps = d_model // 256
    early = 4
    every, front, back = pl.ds(0, d_model), pl.ds(0, early * 256), pl.ds(early * 256, d_model - early * 256)
    parts = {"xy y": (XN, 0, every), "xy dx 0": (XN, 1, front), "xy dx 1": (XN, 1, back), "od y": (OWN, 0, every), "od dx": (OWN, 1, every)}
    pair = {
        name: pltpu.make_async_remote_copy(
            yo.at[pl.ds(first, 2), k, :, cols], yr.at[pl.ds(first, 2), k, :, cols], pair_send.at[i], pair_recv.at[i], device_id=partner, device_id_type=MESH
        )
        for i, (name, (first, k, cols)) in enumerate(parts.items())
    }
    xy = {
        (name, chip): pltpu.make_async_remote_copy(
            xs.at[chip - XN, k, :, cols], xr.at[chip - XN, k, :, cols], xy_send.at[chip - XN, i], xy_recv.at[chip - XN, i], device_id=device_of(chip, 0), device_id_type=MESH
        )
        for i, (name, (first, k, cols)) in enumerate(parts.items())
        if first == XN
        for chip in (XN, YN)
    }

    def send_xy(name):
        _, k, cols = parts[name]
        pair[name].wait_recv()
        for chip in (XN, YN):
            xs[chip - XN, k, :, cols] = (ys[chip, k, :, cols] + yr[chip, k, :, cols].astype(F32)).astype(BF16)
            xy[(name, chip)].start()


    wait_recv(to_partner[:2])
    u_pass(0, 2 * tok, 0, unroll, first=True)
    start_w(0, local_exp, slice(2, 3))
    u_pass(0, 2 * tok, unroll, local_exp, first=True)
    to_chip[XN][2].start()
    to_chip[YN][2].start()
    pass_on((1, 0))
    for e in range(local_exp):
        load_w(e)[2].wait()
    sums_pass(0, (OWN,), 0, 0, steps)

    for chip in (XN, YN):
        wait_recv(forward[chip][:2])
    u_pass(4 * tok, 4 * tok, 0, local_exp)
    pass_on((2,))
    sums_pass(4 * tok, (XN, YN), 0, 0, steps)
    pair["xy y"].start()
    for chip in (XN, YN):
        forward[chip][2].wait_recv()
    dy_pass(4 * tok, 4 * tok, 0, unroll)
    def pass_on_diag(parts):
        for k in parts:
            for copies in relay.values():
                copies[k].wait_recv()
            forward[DIAG][k].start()

    pass_on_diag((1, 0))
    send_xy("xy y")
    dy_pass(4 * tok, 4 * tok, unroll, local_exp)
    pass_on_diag((2,))
    send_gates((XN, YN))
    sums_pass(4 * tok, (XN, YN), 1, 0, early)
    pair["xy dx 0"].start()

    wait_recv(forward[DIAG][:2])
    u_pass(2 * tok, 2 * tok, 0, unroll)
    send_xy("xy dx 0")
    u_pass(2 * tok, 2 * tok, unroll, local_exp)
    to_partner[2].wait_recv()
    forward[DIAG][2].wait_recv()
    dy_pass(0, 4 * tok, 0, local_exp)
    send_gates((OWN, DIAG))

    sums_pass(4 * tok, (XN, YN), 1, early, steps)
    pair["xy dx 1"].start()
    sums_pass(2 * tok, (DIAG,), 0, 0, steps)
    pair["od y"].start()
    send_xy("xy dx 1")

    for c in dg_copies.values():
        c.wait_recv()
    dgate = dgb[0]
    for chip, o in others:
        dgate = dgate + dgr[2 * chip + o]
    own_rt = rt[0:tok, :]
    left = lane < 64
    prob = jnp.where(left, own_rt, 0.0)
    dprob = jnp.where(left & (pltpu.roll(own_rt, 64, 1) >= 0.0), dgate, 0.0)
    dlogit = prob * (dprob - jnp.sum(prob * dprob, axis=1, keepdims=True))
    high = dlogit.astype(BF16)
    low = dlogit - high.astype(F32)
    dlb[0] = jnp.where(left, high.astype(F32), pltpu.roll(low, 64, 1)).astype(BF16)
    start(dl_copies.values())

    sums_pass(0, (OWN, DIAG), 1, 0, steps, transpose=True)
    pair["od dx"].start()
    du_router = dot(dlb[0], wr16[...])
    wait_recv(dl_copies.values())
    dl_out[...] = dlb[...].reshape(8 * tok, LANES)
    for k, base in enumerate((u[0:tok, :].astype(F32), dy[0:tok, :].astype(F32) + du_router)):
        pair[("od y", "od dx")[k]].wait_recv()
        send_out[k] = (ys[DIAG, k] + yr[DIAG, k].astype(F32)).astype(BF16)
        own = ys[OWN, k] + yr[OWN, k].astype(F32) + base
        for (name, chip), copy in xy.items():
            if parts[name][1] == k:
                copy.wait_recv()
        own_out[k] = own + xr[0, k].astype(F32) + xr[1, k].astype(F32)

    for copies in (to_partner, *to_chip.values(), *forward.values(), *relay.values(), dg_copies.values(), dl_copies.values(), pair.values(), xy.values()):
        for c in copies:
            c.wait_send()


def grads_kernel(sizes, xt, dy, ga, d1, d3, dl, dwg_hbm, dwu_hbm, dwd_hbm, dwr_ref, gu, dn, sems):
    local_exp, ffn = sizes

    def copies(e, slot):
        return [
            pltpu.make_async_copy(gu.at[slot, :, pl.ds(0, ffn)], dwg_hbm.at[e], sems.at[0, slot]),
            pltpu.make_async_copy(gu.at[slot, :, pl.ds(ffn, ffn)], dwu_hbm.at[e], sems.at[1, slot]),
            pltpu.make_async_copy(dn.at[slot], dwd_hbm.at[e], sems.at[2, slot]),
        ]

    def one(e, slot):
        cols = pl.ds(pl.multiple_of(e * ffn, ffn), ffn)
        gu[slot] = dot(xt[...], jnp.concatenate([d1[:, cols], d3[:, cols]], axis=1))
        for c in copies(e, slot)[:2]:
            c.start()
        dn[slot] = lax.dot_general(ga[:, cols], dy[...], (((0,), (0,)), ((), ())), preferred_element_type=F32)
        copies(e, slot)[2].start()

    def body(i, carry):
        for slot in (0, 1):

            @pl.when(i > 0)
            def _():
                for c in copies(2 * i + slot - 2, slot):
                    c.wait()

            one(2 * i + slot, slot)
        return carry

    lax.fori_loop(0, local_exp // 2, body, 0)
    wide = dot_t(dl[...].T, xt[...])
    wide = wide[0:64] + wide[64:128]
    for g in range(dwr_ref.shape[0] // local_exp):
        dwr_ref[g * local_exp : (g + 1) * local_exp, :] = wide[g * GROUP : g * GROUP + local_exp]
    for slot in (0, 1):
        for c in copies(local_exp - 2 + slot, slot):
            c.wait()


def solution(mesh):
    tok_spec = P(("dp", "ep", "etp"), None)
    col_spec = P("ep", None, "etp")
    row_spec = P("ep", "etp", None)
    in_specs = (tok_spec, tok_spec, tok_spec, P(None, None), col_spec, col_spec, row_spec)
    out_specs = (tok_spec, tok_spec, P(("dp", "ep"), None, "etp"), P(("dp", "ep"), None, "etp"), P(("dp", "ep"), "etp", None), P("dp", None))

    def device_step(u_loc, dy_loc, ids_loc, w_router, w_gate, w_up, w_down):
        tok, d_model = u_loc.shape
        top_k = ids_loc.shape[1]
        experts = w_router.shape[1]
        local_exp, _, ffn = w_gate.shape
        rows = 8 * tok
        wide = local_exp * ffn
        any_spec = pl.BlockSpec(memory_space=pl.ANY)
        vmem_spec = pl.BlockSpec(memory_space=pltpu.VMEM)
        S = jax.ShapeDtypeStruct
        dma = pltpu.SemaphoreType.DMA
        dy, ga, d1, d3, xt, dl, own, send = pl.pallas_call(
            functools.partial(rows_kernel, (tok, d_model, ffn, local_exp, experts, top_k)),
            name="expert_rows",
            in_specs=[any_spec] * 7,
            out_specs=[vmem_spec] * 8,
            out_shape=[
                pltpu.VMEM((rows, d_model), BF16),
                pltpu.VMEM((rows, wide), BF16), pltpu.VMEM((rows, wide), BF16), pltpu.VMEM((rows, wide), BF16),
                pltpu.VMEM((d_model, rows), BF16), pltpu.VMEM((rows, LANES), BF16),
                pltpu.VMEM((2, tok, d_model), F32), pltpu.VMEM((2, tok, d_model), BF16),
            ],
            scratch_shapes=[
                pltpu.VMEM((rows, d_model), BF16), pltpu.VMEM((top_k, tok), jnp.int32), pltpu.VMEM((experts, d_model), BF16),
                pltpu.VMEM((rows, LANES), F32),
                pltpu.VMEM((d_model, wide), BF16), pltpu.VMEM((d_model, wide), BF16), pltpu.VMEM((wide, d_model), BF16),
                pltpu.VMEM((rows, wide), F32), pltpu.VMEM((2, 4 * tok, ffn), F32),
                pltpu.VMEM((4, 2, tok, d_model), F32),
                pltpu.VMEM((4, 2, tok, d_model), BF16), pltpu.VMEM((4, 2, tok, d_model), BF16),
                pltpu.VMEM((2, 2, tok, d_model), BF16), pltpu.VMEM((2, 2, tok, d_model), BF16),
                pltpu.VMEM((4 * tok, LANES), F32),
                pltpu.VMEM((8, tok, LANES), F32), pltpu.VMEM((8, tok, LANES), F32),
                pltpu.VMEM((8, tok, LANES), BF16),
                pltpu.VMEM((LANES, d_model), BF16),
                dma((4,)), dma((3, local_exp)), dma((3, 8)), dma((3, 8)), dma((16,)), dma((16,)),
                dma((5,)), dma((5,)), dma((2, 3)), dma((2, 3)),
            ],
            compiler_params=pltpu.CompilerParams(collective_id=0, has_side_effects=True, vmem_limit_bytes=48 * 1024 * 1024),
        )(u_loc, dy_loc, ids_loc.T, w_router.T, w_gate, w_up, w_down)

        n_ep, n_etp = lax.axis_size("ep"), lax.axis_size("etp")
        got = lax.ppermute(send, ("etp", "ep"), [(i, i ^ (n_ep + 2)) for i in range(n_ep * n_etp)])

        kept = [pltpu.with_memory_space_constraint(a, pltpu.VMEM) for a in (xt, dy, ga, d1, d3, dl)]
        dwg, dwu, dwd, dwr = pl.pallas_call(
            functools.partial(grads_kernel, (local_exp, ffn)),
            name="weight_grads",
            in_specs=[vmem_spec] * 6,
            out_specs=[any_spec] * 3 + [vmem_spec],
            out_shape=[S((local_exp, d_model, ffn), F32), S((local_exp, d_model, ffn), F32), S((local_exp, ffn, d_model), F32), S((experts, d_model), F32)],
            scratch_shapes=[pltpu.VMEM((2, d_model, 2 * ffn), F32), pltpu.VMEM((2, ffn, d_model), F32), dma((3, 2))],
            compiler_params=pltpu.CompilerParams(vmem_limit_bytes=24 * 1024 * 1024),
            cost_estimate=pl.CostEstimate(flops=3 * 2 * rows * wide * d_model, bytes_accessed=12 * wide * d_model + 10 * rows * wide, transcendentals=0),
        )(*kept)

        y_loc = (own[0] + got[0].astype(F32)).astype(BF16)
        du_loc = (own[1] + got[1].astype(F32)).astype(BF16)
        return y_loc, du_loc, dwg, dwu, dwd, dwr.T

    return jax.shard_map(device_step, mesh=mesh, in_specs=in_specs, out_specs=out_specs, check_vma=False)
```

```python
import functools

import jax
import jax.numpy as jnp
from jax import lax
from jax.experimental import pallas as pl
from jax.experimental.pallas import tpu as pltpu
from jax.sharding import PartitionSpec as P

MESH = pl.DeviceIdType.MESH
F32 = jnp.float32
BF16 = jnp.bfloat16
LANES = 128
GROUP = 16
OWN, DIAG, XN, YN = 0, 1, 2, 3


def dot(a, b):
    return jnp.dot(a, b, preferred_element_type=F32)


def dot_t(a, b):
    return lax.dot_general(a, b, (((1,), (1,)), ((), ())), preferred_element_type=F32)


def flip(index, bit):
    return index + bit - 2 * index * bit


def over_tokens(a, b):
    return lax.dot_general(a, b, (((0,), (0,)), ((), ())), preferred_element_type=F32)


def device_of(chip, other):
    ep, etp = lax.axis_index("ep"), lax.axis_index("etp")
    xb, yb = {OWN: (0, 0), DIAG: (1, 1), XN: (1, 0), YN: (0, 1)}[chip]
    return {"dp": lax.axis_index("dp"), "etp": flip(etp, yb), "ep": flip(ep // 2, xb) * 2 + flip(ep % 2, other)}


def rows_kernel(
    sizes, u_hbm, dy_hbm, ids_hbm, wr_hbm, wg_hbm, wu_hbm, wd_hbm,
    dy, ga, d1, d3, xt, gu0, dn0, dl_out, own_out, send_out,
    u, ids_ref, wr_ref, rt, w1, w3, w2, sg, das, ys, yo, yr, xs, xr, dgacc, dgb, dgr, dlb, wr16,
    in_sem, w_sem, ag_send, ag_recv, small_send, small_recv, pair_send, pair_recv, xy_send, xy_recv,
):
    tok, d_model, ffn, local_exp, experts, top_k = sizes
    ep = lax.axis_index("ep")

    load_rows = [pltpu.make_async_copy(src, dst.at[pl.ds(0, tok), :], in_sem.at[k]) for k, (src, dst) in enumerate(((u_hbm, u), (dy_hbm, dy)))]
    load_small = [pltpu.make_async_copy(src, dst, in_sem.at[2 + k]) for k, (src, dst) in enumerate(((wr_hbm, wr_ref), (ids_hbm, ids_ref)))]
    for c in load_rows + load_small:
        c.start()

    def load_w(e):
        cols = pl.ds(pl.multiple_of(e * ffn, ffn), ffn)
        return [
            pltpu.make_async_copy(wg_hbm.at[e], w1.at[:, cols], w_sem.at[0, e]),
            pltpu.make_async_copy(wu_hbm.at[e], w3.at[:, cols], w_sem.at[1, e]),
            pltpu.make_async_copy(wd_hbm.at[e], w2.at[cols, :], w_sem.at[2, e]),
        ]

    unroll = 5

    def start_w(lo, hi, which):
        for e in range(lo, hi):
            for c in load_w(e)[which]:
                c.start()

    start_w(0, 1, slice(0, 2))

    barrier = pltpu.get_barrier_semaphore()
    others = [(chip, o) for chip in (OWN, DIAG, XN, YN) for o in (0, 1) if (chip, o) != (OWN, 0)]
    for chip, o in others:
        pl.semaphore_signal(barrier, inc=1, device_id=device_of(chip, o), device_id_type=MESH)

    def block(chip, o):
        return pl.ds((2 * chip + o) * tok, tok)

    def gather(i, src, dst, dev):
        return [
            pltpu.make_async_remote_copy(ref.at[src, :], ref.at[dst, :], ag_send.at[k, i], ag_recv.at[k, i], device_id=dev, device_id_type=MESH)
            for k, ref in enumerate((rt, u, dy))
        ]

    partner = device_of(OWN, 1)
    to_partner = gather(0, block(OWN, 0), block(OWN, 1), partner)
    to_chip = {chip: gather(chip, block(OWN, 0), block(chip, 0), device_of(chip, 0)) for chip in (XN, YN)}
    forward = {chip: gather(3 + chip, block(chip, 0), block(chip, 1), partner) for chip in (DIAG, XN, YN)}
    half = tok // 2

    def half_of(chip, h):
        return pl.ds(2 * chip * tok + h * half, half)

    relay = {
        YN: gather(1, half_of(YN, 1), half_of(DIAG, 1), device_of(XN, 0)),
        XN: gather(7, half_of(XN, 0), half_of(DIAG, 0), device_of(YN, 0)),
    }

    def start(copies):
        for c in copies:
            c.start()

    def wait_recv(copies):
        for c in copies:
            c.wait_recv()

    def send_part(k, chips):
        for copies in chips:
            copies[k].start()

    first_chips = (to_partner, to_chip[XN], to_chip[YN])
    for c in load_rows:
        c.wait()
    start_w(1, local_exp, slice(0, 2))
    pl.semaphore_wait(barrier, len(others))
    send_part(1, first_chips)

    slot40 = lax.broadcasted_iota(jnp.int32, (LANES, experts), 0) % 64
    col40 = lax.broadcasted_iota(jnp.int32, (LANES, experts), 1)
    spread = (col40 == (slot40 // GROUP) * local_exp + slot40 % GROUP) & (slot40 % GROUP < local_exp)
    for c in load_small:
        c.wait()
    wr16[...] = dot(jnp.where(spread, 1.0, 0.0).astype(BF16), wr_ref[...]).astype(BF16)
    slot_t = lax.broadcasted_iota(jnp.int32, (LANES, tok), 0) % 64
    expert_t = jnp.where(slot_t % GROUP < local_exp, (slot_t // GROUP) * local_exp + slot_t % GROUP, -1)
    chosen_t = jnp.zeros((LANES, tok), F32)
    for j in range(top_k):
        chosen_t = jnp.where(expert_t == ids_ref[j : j + 1, :], 1.0, chosen_t)
    chosen = chosen_t.T > 0.5
    lane = lax.broadcasted_iota(jnp.int32, (tok, LANES), 1)
    valid = lane % GROUP < local_exp
    logits = jnp.where(valid, dot_t(u[0:tok, :], wr16[...]), -1e30)
    top = jnp.max(logits, axis=1, keepdims=True)
    expo = jnp.where(valid, jnp.exp(logits - top), 0.0)
    prob = expo / jnp.sum(jnp.where(lane < 64, expo, 0.0), axis=1, keepdims=True)
    rt[0:tok, :] = jnp.where((lane < 64) | chosen, prob, -1.0)
    send_part(0, first_chips)
    to_partner[2].start()

    def pass_on(parts):
        for chip in (XN, YN):
            for k in parts:
                to_chip[chip][k].wait_recv()
                relay[chip][k].start()
                forward[chip][k].start()

    def cols_of(e):
        return pl.ds(pl.multiple_of(e * ffn, ffn), ffn)

    def gate_of(rows, count, e):
        lanes = lax.broadcasted_iota(jnp.int32, (count, LANES), 1)
        return jnp.sum(jnp.where(lanes == 64 + ep * GROUP + e, rt[rows, :], 0.0), axis=1, keepdims=True)

    def over_experts(lo, hi, one, which=None):
        def body(i, carry):
            if which is not None:
                for k in range(unroll):
                    for c in load_w(i * unroll + k)[which]:
                        c.wait()
            for k in range(unroll):
                one(i * unroll + k, k % 2)
            return carry

        lax.fori_loop(lo // unroll, hi // unroll, body, 0)

    def u_pass(row, count, lo, hi, first=False):
        rows = pl.ds(row, count)

        def one(e, slot):
            cols = cols_of(e)
            gate = gate_of(rows, count, e)
            on = gate >= 0.0
            h1 = jnp.where(on, dot(u[rows, :], w1[:, cols]), 0.0).astype(BF16)
            h3 = jnp.where(on, dot(u[rows, :], w3[:, cols]), 0.0).astype(BF16)
            d1[rows, cols] = h1
            d3[rows, cols] = h3
            h1 = h1.astype(F32)
            sig = jax.nn.sigmoid(h1)
            sg[rows, cols] = sig
            act = (h1 * sig * h3.astype(F32)).astype(BF16).astype(F32)
            ga[rows, cols] = (gate * act).astype(BF16)

        over_experts(lo, hi, one, slice(0, 2) if first else None)

    def dy_pass(row, count, lo, hi):
        rows = pl.ds(row, count)
        if lo == 0:
            dgacc[...] = jnp.zeros_like(dgacc)

        def one(e, slot):
            cols = cols_of(e)
            das[slot, 0:count, :] = dot_t(dy[rows, :], w2[cols, :])
            for at in range(0, count, tok):
                part = pl.ds(row + at, tok)
                lanes = lax.broadcasted_iota(jnp.int32, (tok, LANES), 1)
                gate = gate_of(part, tok, e)
                h1 = d1[part, cols].astype(F32)
                h3 = d3[part, cols].astype(F32)
                sig = sg[part, cols]
                silu = h1 * sig
                da = das[slot, at : at + tok, :]
                act = (silu * h3).astype(BF16).astype(F32)
                dgate = jnp.sum(act * da, axis=1, keepdims=True)
                dgacc[at : at + tok, :] = jnp.where(lanes == ep * GROUP + e, dgate, dgacc[at : at + tok, :])
                da = jnp.where(gate >= 0.0, gate * da, 0.0).astype(BF16).astype(F32)
                d1[part, cols] = (da * h3 * (sig + silu - silu * sig)).astype(BF16)
                d3[part, cols] = (da * silu).astype(BF16)

        over_experts(lo, hi, one)

    def small(i, src, dst, dev):
        return pltpu.make_async_remote_copy(src, dst, small_send.at[i], small_recv.at[i], device_id=dev, device_id_type=MESH)

    dg_copies = {(chip, o): small(2 * chip + o, dgb.at[2 * chip + o], dgr.at[2 * chip + o], device_of(chip, o)) for chip, o in others}
    dl_copies = {(chip, o): small(8 + 2 * chip + o, dlb.at[0], dlb.at[2 * chip + o], device_of(chip, o)) for chip, o in others}

    def send_gates(chips):
        for i, chip in enumerate(chips):
            for o in (0, 1):
                k = 2 * i + o
                dgb[2 * chip + o] = dgacc[k * tok : (k + 1) * tok, :]
                if (chip, o) != (OWN, 0):
                    dg_copies[(chip, o)].start()

    def sums_pass(row, chips, k, lo, hi, transpose=False):
        rows = pl.ds(row, 2 * tok * len(chips))
        width = 256
        for n in range(lo, hi):
            cols = pl.ds(n * width, width)
            tile = dot(ga[rows, :], w2[:, cols]) if k == 0 else dot_t(d1[rows, :], w1[cols, :]) + dot_t(d3[rows, :], w3[cols, :])
            if transpose:
                xt[cols, :] = u[:, cols].T
            for i, chip in enumerate(chips):
                at = 2 * tok * i
                ys[chip, k, :, cols] = tile[at : at + tok]
                yo[chip, k, :, cols] = tile[at + tok : at + 2 * tok].astype(BF16)

    steps = d_model // 256
    early = 4
    every, front, back = pl.ds(0, d_model), pl.ds(0, early * 256), pl.ds(early * 256, d_model - early * 256)
    parts = {"xy y": (XN, 0, every), "xy dx 0": (XN, 1, front), "xy dx 1": (XN, 1, back), "od y": (OWN, 0, every), "od dx": (OWN, 1, every)}
    pair = {
        name: pltpu.make_async_remote_copy(
            yo.at[pl.ds(first, 2), k, :, cols], yr.at[pl.ds(first, 2), k, :, cols], pair_send.at[i], pair_recv.at[i], device_id=partner, device_id_type=MESH
        )
        for i, (name, (first, k, cols)) in enumerate(parts.items())
    }
    xy = {
        (name, chip): pltpu.make_async_remote_copy(
            xs.at[chip - XN, k, :, cols], xr.at[chip - XN, k, :, cols], xy_send.at[chip - XN, i], xy_recv.at[chip - XN, i], device_id=device_of(chip, 0), device_id_type=MESH
        )
        for i, (name, (first, k, cols)) in enumerate(parts.items())
        if first == XN
        for chip in (XN, YN)
    }

    def send_xy(name):
        _, k, cols = parts[name]
        pair[name].wait_recv()
        for chip in (XN, YN):
            xs[chip - XN, k, :, cols] = (ys[chip, k, :, cols] + yr[chip, k, :, cols].astype(F32)).astype(BF16)
            xy[(name, chip)].start()


    wait_recv(to_partner[:2])
    u_pass(0, 2 * tok, 0, unroll, first=True)
    start_w(0, local_exp, slice(2, 3))
    u_pass(0, 2 * tok, unroll, local_exp, first=True)
    to_chip[XN][2].start()
    to_chip[YN][2].start()
    pass_on((1, 0))
    for e in range(local_exp):
        load_w(e)[2].wait()
    sums_pass(0, (OWN,), 0, 0, steps)

    for chip in (XN, YN):
        wait_recv(forward[chip][:2])
    u_pass(4 * tok, 4 * tok, 0, local_exp)
    pass_on((2,))
    sums_pass(4 * tok, (XN, YN), 0, 0, steps)
    pair["xy y"].start()
    for chip in (XN, YN):
        forward[chip][2].wait_recv()
    dy_pass(4 * tok, 4 * tok, 0, unroll)
    def pass_on_diag(parts):
        for k in parts:
            for copies in relay.values():
                copies[k].wait_recv()
            forward[DIAG][k].start()

    pass_on_diag((1, 0))
    send_xy("xy y")
    dy_pass(4 * tok, 4 * tok, unroll, local_exp)
    pass_on_diag((2,))
    send_gates((XN, YN))
    sums_pass(4 * tok, (XN, YN), 1, 0, early)
    pair["xy dx 0"].start()

    wait_recv(forward[DIAG][:2])
    u_pass(2 * tok, 2 * tok, 0, unroll)
    send_xy("xy dx 0")
    u_pass(2 * tok, 2 * tok, unroll, local_exp)
    to_partner[2].wait_recv()
    forward[DIAG][2].wait_recv()
    dy_pass(0, 4 * tok, 0, local_exp)
    send_gates((OWN, DIAG))

    sums_pass(4 * tok, (XN, YN), 1, early, steps)
    pair["xy dx 1"].start()
    sums_pass(2 * tok, (DIAG,), 0, 0, steps)
    pair["od y"].start()
    send_xy("xy dx 1")

    dn0[...] = over_tokens(ga[:, 0:ffn], dy[...])

    for c in dg_copies.values():
        c.wait_recv()
    dgate = dgb[0]
    for chip, o in others:
        dgate = dgate + dgr[2 * chip + o]
    own_rt = rt[0:tok, :]
    left = lane < 64
    prob = jnp.where(left, own_rt, 0.0)
    dprob = jnp.where(left & (pltpu.roll(own_rt, 64, 1) >= 0.0), dgate, 0.0)
    dlogit = prob * (dprob - jnp.sum(prob * dprob, axis=1, keepdims=True))
    high = dlogit.astype(BF16)
    low = dlogit - high.astype(F32)
    dlb[0] = jnp.where(left, high.astype(F32), pltpu.roll(low, 64, 1)).astype(BF16)
    start(dl_copies.values())

    sums_pass(0, (OWN, DIAG), 1, 0, steps, transpose=True)
    pair["od dx"].start()
    gu0[...] = dot(xt[...], jnp.concatenate([d1[:, 0:ffn], d3[:, 0:ffn]], axis=1))
    du_router = dot(dlb[0], wr16[...])
    wait_recv(dl_copies.values())
    dl_out[...] = dlb[...].reshape(8 * tok, LANES)
    for k, base in enumerate((u[0:tok, :].astype(F32), dy[0:tok, :].astype(F32) + du_router)):
        pair[("od y", "od dx")[k]].wait_recv()
        send_out[k] = (ys[DIAG, k] + yr[DIAG, k].astype(F32)).astype(BF16)
        own = ys[OWN, k] + yr[OWN, k].astype(F32) + base
        for (name, chip), copy in xy.items():
            if parts[name][1] == k:
                copy.wait_recv()
        own_out[k] = own + xr[0, k].astype(F32) + xr[1, k].astype(F32)

    for copies in (to_partner, *to_chip.values(), *forward.values(), *relay.values(), dg_copies.values(), dl_copies.values(), pair.values(), xy.values()):
        for c in copies:
            c.wait_send()


def grads_kernel(sizes, xt, dy, ga, d1, d3, gu0, dn0, dl, dwg_hbm, dwu_hbm, dwd_hbm, dwr_ref, gu, dn, sems):
    local_exp, ffn = sizes

    def copies(e, slot, wide=None, deep=None):
        wide = gu.at[slot] if wide is None else wide
        deep = dn.at[slot] if deep is None else deep
        return [
            pltpu.make_async_copy(wide.at[:, pl.ds(0, ffn)], dwg_hbm.at[e], sems.at[0, slot]),
            pltpu.make_async_copy(wide.at[:, pl.ds(ffn, ffn)], dwu_hbm.at[e], sems.at[1, slot]),
            pltpu.make_async_copy(deep, dwd_hbm.at[e], sems.at[2, slot]),
        ]

    def columns(e):
        return pl.ds(pl.multiple_of(e * ffn, ffn), ffn)

    def make_wide(e, slot):
        gu[slot] = dot(xt[...], jnp.concatenate([d1[:, columns(e)], d3[:, columns(e)]], axis=1))

    def make_deep(e, slot):
        dn[slot] = over_tokens(ga[:, columns(e)], dy[...])

    def start(e, slot, which=slice(0, 3)):
        for c in copies(e, slot)[which]:
            c.start()

    def wait(e, slot):
        for c in copies(e, slot):
            c.wait()

    first = copies(0, 4, gu0, dn0)
    for c in first:
        c.start()

    def body(i, carry):
        e, slot = 1 + 2 * i, 2 * (i % 2)

        @pl.when(i >= 2)
        def _():
            for k in (0, 1):
                wait(e + k - 4, slot + k)

        for k in (0, 1):
            make_wide(e + k, slot + k)
            make_deep(e + k, slot + k)
        for k in (0, 1):
            start(e + k, slot + k)
        return carry

    rounds = (local_exp - 1) // 2
    lax.fori_loop(0, rounds, body, 0)
    made = [(1 + 2 * i + k, 2 * (i % 2) + k) for i in range(rounds) for k in (0, 1)]
    if local_exp % 2 == 0:
        e, slot = local_exp - 1, 2 * (rounds % 2)
        wait(e - 4, slot)
        make_wide(e, slot)
        start(e, slot, slice(0, 2))
        make_deep(e, slot)
        start(e, slot, slice(2, 3))
        made = made[-3:] + [(e, slot)]
    else:
        made = made[-4:]
    folded = dot_t(dl[...].T, xt[...])
    folded = folded[0:64] + folded[64:128]
    for g in range(dwr_ref.shape[0] // local_exp):
        dwr_ref[g * local_exp : (g + 1) * local_exp, :] = folded[g * GROUP : g * GROUP + local_exp]
    for e, slot in made:
        wait(e, slot)
    for c in first:
        c.wait()


def solution(mesh):
    tok_spec = P(("dp", "ep", "etp"), None)
    col_spec = P("ep", None, "etp")
    row_spec = P("ep", "etp", None)
    in_specs = (tok_spec, tok_spec, tok_spec, P(None, None), col_spec, col_spec, row_spec)
    out_specs = (tok_spec, tok_spec, P(("dp", "ep"), None, "etp"), P(("dp", "ep"), None, "etp"), P(("dp", "ep"), "etp", None), P("dp", None))

    def device_step(u_loc, dy_loc, ids_loc, w_router, w_gate, w_up, w_down):
        tok, d_model = u_loc.shape
        top_k = ids_loc.shape[1]
        experts = w_router.shape[1]
        local_exp, _, ffn = w_gate.shape
        rows = 8 * tok
        wide = local_exp * ffn
        any_spec = pl.BlockSpec(memory_space=pl.ANY)
        vmem_spec = pl.BlockSpec(memory_space=pltpu.VMEM)
        S = jax.ShapeDtypeStruct
        dma = pltpu.SemaphoreType.DMA
        dy, ga, d1, d3, xt, gu0, dn0, dl, own, send = pl.pallas_call(
            functools.partial(rows_kernel, (tok, d_model, ffn, local_exp, experts, top_k)),
            name="expert_rows",
            in_specs=[any_spec] * 7,
            out_specs=[vmem_spec] * 10,
            out_shape=[
                pltpu.VMEM((rows, d_model), BF16),
                pltpu.VMEM((rows, wide), BF16), pltpu.VMEM((rows, wide), BF16), pltpu.VMEM((rows, wide), BF16),
                pltpu.VMEM((d_model, rows), BF16), pltpu.VMEM((d_model, 2 * ffn), F32), pltpu.VMEM((ffn, d_model), F32), pltpu.VMEM((rows, LANES), BF16),
                pltpu.VMEM((2, tok, d_model), F32), pltpu.VMEM((2, tok, d_model), BF16),
            ],
            scratch_shapes=[
                pltpu.VMEM((rows, d_model), BF16), pltpu.VMEM((top_k, tok), jnp.int32), pltpu.VMEM((experts, d_model), BF16),
                pltpu.VMEM((rows, LANES), F32),
                pltpu.VMEM((d_model, wide), BF16), pltpu.VMEM((d_model, wide), BF16), pltpu.VMEM((wide, d_model), BF16),
                pltpu.VMEM((rows, wide), F32), pltpu.VMEM((2, 4 * tok, ffn), F32),
                pltpu.VMEM((4, 2, tok, d_model), F32),
                pltpu.VMEM((4, 2, tok, d_model), BF16), pltpu.VMEM((4, 2, tok, d_model), BF16),
                pltpu.VMEM((2, 2, tok, d_model), BF16), pltpu.VMEM((2, 2, tok, d_model), BF16),
                pltpu.VMEM((4 * tok, LANES), F32),
                pltpu.VMEM((8, tok, LANES), F32), pltpu.VMEM((8, tok, LANES), F32),
                pltpu.VMEM((8, tok, LANES), BF16),
                pltpu.VMEM((LANES, d_model), BF16),
                dma((4,)), dma((3, local_exp)), dma((3, 8)), dma((3, 8)), dma((16,)), dma((16,)),
                dma((5,)), dma((5,)), dma((2, 3)), dma((2, 3)),
            ],
            compiler_params=pltpu.CompilerParams(collective_id=0, has_side_effects=True, vmem_limit_bytes=43 * 1024 * 1024),
        )(u_loc, dy_loc, ids_loc.T, w_router.T, w_gate, w_up, w_down)

        n_ep, n_etp = lax.axis_size("ep"), lax.axis_size("etp")
        got = lax.ppermute(send, ("etp", "ep"), [(i, i ^ (n_ep + 2)) for i in range(n_ep * n_etp)])

        kept = [pltpu.with_memory_space_constraint(a, pltpu.VMEM) for a in (xt, dy, ga, d1, d3, gu0, dn0, dl)]
        dwg, dwu, dwd, dwr = pl.pallas_call(
            functools.partial(grads_kernel, (local_exp, ffn)),
            name="weight_grads",
            in_specs=[vmem_spec] * 8,
            out_specs=[any_spec] * 3 + [vmem_spec],
            out_shape=[S((local_exp, d_model, ffn), F32), S((local_exp, d_model, ffn), F32), S((local_exp, ffn, d_model), F32), S((experts, d_model), F32)],
            scratch_shapes=[pltpu.VMEM((4, d_model, 2 * ffn), F32), pltpu.VMEM((4, ffn, d_model), F32), dma((3, 5))],
            compiler_params=pltpu.CompilerParams(vmem_limit_bytes=30 * 1024 * 1024),
            cost_estimate=pl.CostEstimate(flops=3 * 2 * rows * wide * d_model, bytes_accessed=12 * wide * d_model + 10 * rows * wide, transcendentals=0),
        )(*kept)

        y_loc = (own[0] + got[0].astype(F32)).astype(BF16)
        du_loc = (own[1] + got[1].astype(F32)).astype(BF16)
        return y_loc, du_loc, dwg, dwu, dwd, dwr.T

    return jax.shard_map(device_step, mesh=mesh, in_specs=in_specs, out_specs=out_specs, check_vma=False)
```

```python
import functools

import jax
import jax.numpy as jnp
from jax import lax
from jax.experimental import pallas as pl
from jax.experimental.pallas import tpu as pltpu
from jax.sharding import PartitionSpec as P

MESH = pl.DeviceIdType.MESH
F32 = jnp.float32
BF16 = jnp.bfloat16
LANES = 128
GROUP = 16
OWN, DIAG, XN, YN = 0, 1, 2, 3


def dot(a, b):
    return jnp.dot(a, b, preferred_element_type=F32)


def dot_t(a, b):
    return lax.dot_general(a, b, (((1,), (1,)), ((), ())), preferred_element_type=F32)


def flip(index, bit):
    return index + bit - 2 * index * bit


def over_tokens(a, b):
    return lax.dot_general(a, b, (((0,), (0,)), ((), ())), preferred_element_type=F32)


def device_of(chip, other):
    ep, etp = lax.axis_index("ep"), lax.axis_index("etp")
    xb, yb = {OWN: (0, 0), DIAG: (1, 1), XN: (1, 0), YN: (0, 1)}[chip]
    return {"dp": lax.axis_index("dp"), "etp": flip(etp, yb), "ep": flip(ep // 2, xb) * 2 + flip(ep % 2, other)}


def rows_kernel(
    sizes, u_hbm, dy_hbm, ids_hbm, wr_hbm, wg_hbm, wu_hbm, wd_hbm,
    dy, ga, d1, d3, xt, gu0, dn0, dl_out, own_out, send_out,
    u, ids_ref, wr_ref, rt, w1, w3, w2, sg, das, ys, yo, yr, xs, xr, dgacc, dgb, dgr, dlb, wr16,
    in_sem, w_sem, ag_send, ag_recv, small_send, small_recv, pair_send, pair_recv, xy_send, xy_recv,
):
    tok, d_model, ffn, local_exp, experts, top_k = sizes
    ep = lax.axis_index("ep")

    load_rows = [pltpu.make_async_copy(src, dst.at[pl.ds(0, tok), :], in_sem.at[k]) for k, (src, dst) in enumerate(((u_hbm, u), (dy_hbm, dy)))]
    load_small = [pltpu.make_async_copy(src, dst, in_sem.at[2 + k]) for k, (src, dst) in enumerate(((wr_hbm, wr_ref), (ids_hbm, ids_ref)))]
    for c in load_rows + load_small:
        c.start()

    def load_w(e):
        cols = pl.ds(pl.multiple_of(e * ffn, ffn), ffn)
        return [
            pltpu.make_async_copy(wg_hbm.at[e], w1.at[:, cols], w_sem.at[0, e]),
            pltpu.make_async_copy(wu_hbm.at[e], w3.at[:, cols], w_sem.at[1, e]),
            pltpu.make_async_copy(wd_hbm.at[e], w2.at[cols, :], w_sem.at[2, e]),
        ]

    unroll = 5

    def start_w(lo, hi, which):
        for e in range(lo, hi):
            for c in load_w(e)[which]:
                c.start()

    start_w(0, 3, slice(0, 2))

    barrier = pltpu.get_barrier_semaphore()
    others = [(chip, o) for chip in (OWN, DIAG, XN, YN) for o in (0, 1) if (chip, o) != (OWN, 0)]
    for chip, o in others:
        pl.semaphore_signal(barrier, inc=1, device_id=device_of(chip, o), device_id_type=MESH)

    def block(chip, o):
        return pl.ds((2 * chip + o) * tok, tok)

    def gather(i, src, dst, dev):
        return [
            pltpu.make_async_remote_copy(ref.at[src, :], ref.at[dst, :], ag_send.at[k, i], ag_recv.at[k, i], device_id=dev, device_id_type=MESH)
            for k, ref in enumerate((rt, u, dy))
        ]

    partner = device_of(OWN, 1)
    to_partner = gather(0, block(OWN, 0), block(OWN, 1), partner)
    to_chip = {chip: gather(chip, block(OWN, 0), block(chip, 0), device_of(chip, 0)) for chip in (XN, YN)}
    forward = {chip: gather(3 + chip, block(chip, 0), block(chip, 1), partner) for chip in (DIAG, XN, YN)}
    half = tok // 2

    def half_of(chip, h):
        return pl.ds(2 * chip * tok + h * half, half)

    relay = {
        YN: gather(1, half_of(YN, 1), half_of(DIAG, 1), device_of(XN, 0)),
        XN: gather(7, half_of(XN, 0), half_of(DIAG, 0), device_of(YN, 0)),
    }

    def start(copies):
        for c in copies:
            c.start()

    def wait_recv(copies):
        for c in copies:
            c.wait_recv()

    def send_part(k, chips):
        for copies in chips:
            copies[k].start()

    first_chips = (to_partner, to_chip[XN], to_chip[YN])
    for c in load_rows:
        c.wait()
    start_w(3, local_exp, slice(0, 2))
    pl.semaphore_wait(barrier, len(others))
    send_part(1, first_chips)

    slot40 = lax.broadcasted_iota(jnp.int32, (LANES, experts), 0) % 64
    col40 = lax.broadcasted_iota(jnp.int32, (LANES, experts), 1)
    spread = (col40 == (slot40 // GROUP) * local_exp + slot40 % GROUP) & (slot40 % GROUP < local_exp)
    for c in load_small:
        c.wait()
    wr16[...] = dot(jnp.where(spread, 1.0, 0.0).astype(BF16), wr_ref[...]).astype(BF16)
    slot_t = lax.broadcasted_iota(jnp.int32, (LANES, tok), 0) % 64
    expert_t = jnp.where(slot_t % GROUP < local_exp, (slot_t // GROUP) * local_exp + slot_t % GROUP, -1)
    chosen_t = jnp.zeros((LANES, tok), F32)
    for j in range(top_k):
        chosen_t = jnp.where(expert_t == ids_ref[j : j + 1, :], 1.0, chosen_t)
    chosen = chosen_t.T > 0.5
    lane = lax.broadcasted_iota(jnp.int32, (tok, LANES), 1)
    valid = lane % GROUP < local_exp
    logits = jnp.where(valid, dot_t(u[0:tok, :], wr16[...]), -1e30)
    top = jnp.max(logits, axis=1, keepdims=True)
    expo = jnp.where(valid, jnp.exp(logits - top), 0.0)
    prob = expo / jnp.sum(jnp.where(lane < 64, expo, 0.0), axis=1, keepdims=True)
    rt[0:tok, :] = jnp.where((lane < 64) | chosen, prob, -1.0)
    send_part(0, first_chips)
    to_partner[2].start()

    def pass_on(parts):
        for chip in (XN, YN):
            for k in parts:
                to_chip[chip][k].wait_recv()
                relay[chip][k].start()
                forward[chip][k].start()

    def cols_of(e):
        return pl.ds(pl.multiple_of(e * ffn, ffn), ffn)

    def gate_of(rows, count, e):
        lanes = lax.broadcasted_iota(jnp.int32, (count, LANES), 1)
        return jnp.sum(jnp.where(lanes == 64 + ep * GROUP + e, rt[rows, :], 0.0), axis=1, keepdims=True)

    def over_experts(lo, hi, one, which=None):
        step = unroll if which is not None else hi - lo

        def body(i, carry):
            if which is not None:
                for k in range(step):
                    for c in load_w(lo + i * step + k)[which]:
                        c.wait()
            for k in range(step):
                one(lo + i * step + k, k % 2)
            return carry

        lax.fori_loop(0, (hi - lo) // step, body, 0)

    def u_pass(row, count, lo, hi, first=False):
        rows = pl.ds(row, count)

        def one(e, slot):
            cols = cols_of(e)
            gate = gate_of(rows, count, e)
            on = gate >= 0.0
            h1 = jnp.where(on, dot(u[rows, :], w1[:, cols]), 0.0).astype(BF16)
            h3 = jnp.where(on, dot(u[rows, :], w3[:, cols]), 0.0).astype(BF16)
            d1[rows, cols] = h1
            d3[rows, cols] = h3
            h1 = h1.astype(F32)
            sig = jax.nn.sigmoid(h1)
            sg[rows, cols] = sig
            act = (h1 * sig * h3.astype(F32)).astype(BF16).astype(F32)
            ga[rows, cols] = (gate * act).astype(BF16)

        over_experts(lo, hi, one, slice(0, 2) if first else None)

    def dy_pass(row, count, lo, hi):
        rows = pl.ds(row, count)
        if lo == 0:
            dgacc[...] = jnp.zeros_like(dgacc)

        def one(e, slot):
            cols = cols_of(e)
            das[slot, 0:count, :] = dot_t(dy[rows, :], w2[cols, :])
            for at in range(0, count, tok):
                part = pl.ds(row + at, tok)
                lanes = lax.broadcasted_iota(jnp.int32, (tok, LANES), 1)
                gate = gate_of(part, tok, e)
                h1 = d1[part, cols].astype(F32)
                h3 = d3[part, cols].astype(F32)
                sig = sg[part, cols]
                silu = h1 * sig
                da = das[slot, at : at + tok, :]
                act = (silu * h3).astype(BF16).astype(F32)
                dgate = jnp.sum(act * da, axis=1, keepdims=True)
                dgacc[at : at + tok, :] = jnp.where(lanes == ep * GROUP + e, dgate, dgacc[at : at + tok, :])
                da = jnp.where(gate >= 0.0, gate * da, 0.0).astype(BF16).astype(F32)
                d1[part, cols] = (da * h3 * (sig + silu - silu * sig)).astype(BF16)
                d3[part, cols] = (da * silu).astype(BF16)

        over_experts(lo, hi, one)

    def small(i, src, dst, dev):
        return pltpu.make_async_remote_copy(src, dst, small_send.at[i], small_recv.at[i], device_id=dev, device_id_type=MESH)

    dg_copies = {(chip, o): small(2 * chip + o, dgb.at[2 * chip + o], dgr.at[2 * chip + o], device_of(chip, o)) for chip, o in others}
    dl_copies = {(chip, o): small(8 + 2 * chip + o, dlb.at[0], dlb.at[2 * chip + o], device_of(chip, o)) for chip, o in others}

    def send_gates(chips):
        for i, chip in enumerate(chips):
            for o in (0, 1):
                k = 2 * i + o
                dgb[2 * chip + o] = dgacc[k * tok : (k + 1) * tok, :]
                if (chip, o) != (OWN, 0):
                    dg_copies[(chip, o)].start()

    def sums_pass(row, chips, k, lo, hi, transpose=False):
        rows = pl.ds(row, 2 * tok * len(chips))
        width = 256
        for n in range(lo, hi):
            cols = pl.ds(n * width, width)
            tile = dot(ga[rows, :], w2[:, cols]) if k == 0 else dot_t(d1[rows, :], w1[cols, :]) + dot_t(d3[rows, :], w3[cols, :])
            if transpose:
                xt[cols, :] = u[:, cols].T
            for i, chip in enumerate(chips):
                at = 2 * tok * i
                ys[chip, k, :, cols] = tile[at : at + tok]
                yo[chip, k, :, cols] = tile[at + tok : at + 2 * tok].astype(BF16)

    steps = d_model // 256
    early = 4
    every, front, back = pl.ds(0, d_model), pl.ds(0, early * 256), pl.ds(early * 256, d_model - early * 256)
    parts = {"xy y": (XN, 0, every), "xy dx 0": (XN, 1, front), "xy dx 1": (XN, 1, back), "od y": (OWN, 0, every), "od dx": (OWN, 1, every)}
    pair = {
        name: pltpu.make_async_remote_copy(
            yo.at[pl.ds(first, 2), k, :, cols], yr.at[pl.ds(first, 2), k, :, cols], pair_send.at[i], pair_recv.at[i], device_id=partner, device_id_type=MESH
        )
        for i, (name, (first, k, cols)) in enumerate(parts.items())
    }
    xy = {
        (name, chip): pltpu.make_async_remote_copy(
            xs.at[chip - XN, k, :, cols], xr.at[chip - XN, k, :, cols], xy_send.at[chip - XN, i], xy_recv.at[chip - XN, i], device_id=device_of(chip, 0), device_id_type=MESH
        )
        for i, (name, (first, k, cols)) in enumerate(parts.items())
        if first == XN
        for chip in (XN, YN)
    }

    def send_xy(name):
        _, k, cols = parts[name]
        pair[name].wait_recv()
        for chip in (XN, YN):
            xs[chip - XN, k, :, cols] = (ys[chip, k, :, cols] + yr[chip, k, :, cols].astype(F32)).astype(BF16)
            xy[(name, chip)].start()


    wait_recv(to_partner[:2])
    u_pass(0, 2 * tok, 0, unroll, first=True)
    start_w(0, local_exp, slice(2, 3))
    u_pass(0, 2 * tok, unroll, local_exp, first=True)
    to_chip[XN][2].start()
    to_chip[YN][2].start()
    pass_on((1, 0))
    for e in range(local_exp):
        load_w(e)[2].wait()
    sums_pass(0, (OWN,), 0, 0, steps)

    for chip in (XN, YN):
        wait_recv(forward[chip][:2])
    u_pass(4 * tok, 4 * tok, 0, local_exp)
    pass_on((2,))
    sums_pass(4 * tok, (XN, YN), 0, 0, steps)
    pair["xy y"].start()
    for chip in (XN, YN):
        forward[chip][2].wait_recv()
    dy_pass(4 * tok, 4 * tok, 0, unroll)
    def pass_on_diag(parts):
        for k in parts:
            for copies in relay.values():
                copies[k].wait_recv()
            forward[DIAG][k].start()

    pass_on_diag((1, 0))
    send_xy("xy y")
    dy_pass(4 * tok, 4 * tok, unroll, local_exp)
    pass_on_diag((2,))
    send_gates((XN, YN))
    sums_pass(4 * tok, (XN, YN), 1, 0, early)
    pair["xy dx 0"].start()

    wait_recv(forward[DIAG][:2])
    u_pass(2 * tok, 2 * tok, 0, unroll)
    send_xy("xy dx 0")
    u_pass(2 * tok, 2 * tok, unroll, local_exp)
    to_partner[2].wait_recv()
    forward[DIAG][2].wait_recv()
    dy_pass(0, 4 * tok, 0, local_exp)
    send_gates((OWN, DIAG))

    sums_pass(4 * tok, (XN, YN), 1, early, steps)
    pair["xy dx 1"].start()
    sums_pass(2 * tok, (DIAG,), 0, 0, steps)
    pair["od y"].start()
    send_xy("xy dx 1")

    dn0[...] = over_tokens(ga[:, 0:ffn], dy[...])

    for c in dg_copies.values():
        c.wait_recv()
    dgate = dgb[0]
    for chip, o in others:
        dgate = dgate + dgr[2 * chip + o]
    own_rt = rt[0:tok, :]
    left = lane < 64
    prob = jnp.where(left, own_rt, 0.0)
    dprob = jnp.where(left & (pltpu.roll(own_rt, 64, 1) >= 0.0), dgate, 0.0)
    dlogit = prob * (dprob - jnp.sum(prob * dprob, axis=1, keepdims=True))
    high = dlogit.astype(BF16)
    low = dlogit - high.astype(F32)
    dlb[0] = jnp.where(left, high.astype(F32), pltpu.roll(low, 64, 1)).astype(BF16)
    start(dl_copies.values())

    sums_pass(0, (OWN, DIAG), 1, 0, steps, transpose=True)
    pair["od dx"].start()
    gu0[...] = dot(xt[...], jnp.concatenate([d1[:, 0:ffn], d3[:, 0:ffn]], axis=1))
    du_router = dot(dlb[0], wr16[...])
    wait_recv(dl_copies.values())
    dl_out[...] = dlb[...].reshape(8 * tok, LANES)
    for k, base in enumerate((u[0:tok, :].astype(F32), dy[0:tok, :].astype(F32) + du_router)):
        pair[("od y", "od dx")[k]].wait_recv()
        send_out[k] = (ys[DIAG, k] + yr[DIAG, k].astype(F32)).astype(BF16)
        own = ys[OWN, k] + yr[OWN, k].astype(F32) + base
        for (name, chip), copy in xy.items():
            if parts[name][1] == k:
                copy.wait_recv()
        own_out[k] = own + xr[0, k].astype(F32) + xr[1, k].astype(F32)

    for copies in (to_partner, *to_chip.values(), *forward.values(), *relay.values(), dg_copies.values(), dl_copies.values(), pair.values(), xy.values()):
        for c in copies:
            c.wait_send()


def grads_kernel(sizes, xt, dy, ga, d1, d3, gu0, dn0, dl, dwg_hbm, dwu_hbm, dwd_hbm, dwr_ref, gu, dn, sems):
    local_exp, ffn = sizes

    def copies(e, slot, wide=None, deep=None):
        wide = gu.at[slot] if wide is None else wide
        deep = dn.at[slot] if deep is None else deep
        return [
            pltpu.make_async_copy(wide.at[:, pl.ds(0, ffn)], dwg_hbm.at[e], sems.at[0, slot]),
            pltpu.make_async_copy(wide.at[:, pl.ds(ffn, ffn)], dwu_hbm.at[e], sems.at[1, slot]),
            pltpu.make_async_copy(deep, dwd_hbm.at[e], sems.at[2, slot]),
        ]

    def columns(e):
        return pl.ds(pl.multiple_of(e * ffn, ffn), ffn)

    def make_wide(e, slot):
        gu[slot] = dot(xt[...], jnp.concatenate([d1[:, columns(e)], d3[:, columns(e)]], axis=1))

    def make_deep(e, slot):
        dn[slot] = over_tokens(ga[:, columns(e)], dy[...])

    def start(e, slot, which=slice(0, 3)):
        for c in copies(e, slot)[which]:
            c.start()

    def wait(e, slot):
        for c in copies(e, slot):
            c.wait()

    first = copies(0, 4, gu0, dn0)
    for c in first:
        c.start()

    def body(i, carry):
        e, slot = 1 + 2 * i, 2 * (i % 2)

        @pl.when(i >= 2)
        def _():
            for k in (0, 1):
                wait(e + k - 4, slot + k)

        for k in (0, 1):
            make_wide(e + k, slot + k)
            make_deep(e + k, slot + k)
        for k in (0, 1):
            start(e + k, slot + k)
        return carry

    rounds = (local_exp - 1) // 2
    lax.fori_loop(0, rounds, body, 0)
    made = [(1 + 2 * i + k, 2 * (i % 2) + k) for i in range(rounds) for k in (0, 1)]
    if local_exp % 2 == 0:
        e, slot = local_exp - 1, 2 * (rounds % 2)
        wait(e - 4, slot)
        make_wide(e, slot)
        start(e, slot, slice(0, 2))
        make_deep(e, slot)
        start(e, slot, slice(2, 3))
        made = made[-3:] + [(e, slot)]
    else:
        made = made[-4:]
    folded = dot_t(dl[...].T, xt[...])
    folded = folded[0:64] + folded[64:128]
    for g in range(dwr_ref.shape[0] // local_exp):
        dwr_ref[g * local_exp : (g + 1) * local_exp, :] = folded[g * GROUP : g * GROUP + local_exp]
    for e, slot in made:
        wait(e, slot)
    for c in first:
        c.wait()


def solution(mesh):
    tok_spec = P(("dp", "ep", "etp"), None)
    col_spec = P("ep", None, "etp")
    row_spec = P("ep", "etp", None)
    in_specs = (tok_spec, tok_spec, tok_spec, P(None, None), col_spec, col_spec, row_spec)
    out_specs = (tok_spec, tok_spec, P(("dp", "ep"), None, "etp"), P(("dp", "ep"), None, "etp"), P(("dp", "ep"), "etp", None), P("dp", None))

    def device_step(u_loc, dy_loc, ids_loc, w_router, w_gate, w_up, w_down):
        tok, d_model = u_loc.shape
        top_k = ids_loc.shape[1]
        experts = w_router.shape[1]
        local_exp, _, ffn = w_gate.shape
        rows = 8 * tok
        wide = local_exp * ffn
        any_spec = pl.BlockSpec(memory_space=pl.ANY)
        vmem_spec = pl.BlockSpec(memory_space=pltpu.VMEM)
        S = jax.ShapeDtypeStruct
        dma = pltpu.SemaphoreType.DMA
        dy, ga, d1, d3, xt, gu0, dn0, dl, own, send = pl.pallas_call(
            functools.partial(rows_kernel, (tok, d_model, ffn, local_exp, experts, top_k)),
            name="expert_rows",
            in_specs=[any_spec] * 7,
            out_specs=[vmem_spec] * 10,
            out_shape=[
                pltpu.VMEM((rows, d_model), BF16),
                pltpu.VMEM((rows, wide), BF16), pltpu.VMEM((rows, wide), BF16), pltpu.VMEM((rows, wide), BF16),
                pltpu.VMEM((d_model, rows), BF16), pltpu.VMEM((d_model, 2 * ffn), F32), pltpu.VMEM((ffn, d_model), F32), pltpu.VMEM((rows, LANES), BF16),
                pltpu.VMEM((2, tok, d_model), F32), pltpu.VMEM((2, tok, d_model), BF16),
            ],
            scratch_shapes=[
                pltpu.VMEM((rows, d_model), BF16), pltpu.VMEM((top_k, tok), jnp.int32), pltpu.VMEM((experts, d_model), BF16),
                pltpu.VMEM((rows, LANES), F32),
                pltpu.VMEM((d_model, wide), BF16), pltpu.VMEM((d_model, wide), BF16), pltpu.VMEM((wide, d_model), BF16),
                pltpu.VMEM((rows, wide), F32), pltpu.VMEM((2, 4 * tok, ffn), F32),
                pltpu.VMEM((4, 2, tok, d_model), F32),
                pltpu.VMEM((4, 2, tok, d_model), BF16), pltpu.VMEM((4, 2, tok, d_model), BF16),
                pltpu.VMEM((2, 2, tok, d_model), BF16), pltpu.VMEM((2, 2, tok, d_model), BF16),
                pltpu.VMEM((4 * tok, LANES), F32),
                pltpu.VMEM((8, tok, LANES), F32), pltpu.VMEM((8, tok, LANES), F32),
                pltpu.VMEM((8, tok, LANES), BF16),
                pltpu.VMEM((LANES, d_model), BF16),
                dma((4,)), dma((3, local_exp)), dma((3, 8)), dma((3, 8)), dma((16,)), dma((16,)),
                dma((5,)), dma((5,)), dma((2, 3)), dma((2, 3)),
            ],
            compiler_params=pltpu.CompilerParams(collective_id=0, has_side_effects=True, vmem_limit_bytes=43 * 1024 * 1024),
        )(u_loc, dy_loc, ids_loc.T, w_router.T, w_gate, w_up, w_down)

        n_ep, n_etp = lax.axis_size("ep"), lax.axis_size("etp")
        got = lax.ppermute(send, ("etp", "ep"), [(i, i ^ (n_ep + 2)) for i in range(n_ep * n_etp)])

        kept = [pltpu.with_memory_space_constraint(a, pltpu.VMEM) for a in (xt, dy, ga, d1, d3, gu0, dn0, dl)]
        dwg, dwu, dwd, dwr = pl.pallas_call(
            functools.partial(grads_kernel, (local_exp, ffn)),
            name="weight_grads",
            in_specs=[vmem_spec] * 8,
            out_specs=[any_spec] * 3 + [vmem_spec],
            out_shape=[S((local_exp, d_model, ffn), F32), S((local_exp, d_model, ffn), F32), S((local_exp, ffn, d_model), F32), S((experts, d_model), F32)],
            scratch_shapes=[pltpu.VMEM((4, d_model, 2 * ffn), F32), pltpu.VMEM((4, ffn, d_model), F32), dma((3, 5))],
            compiler_params=pltpu.CompilerParams(vmem_limit_bytes=30 * 1024 * 1024),
            cost_estimate=pl.CostEstimate(flops=3 * 2 * rows * wide * d_model, bytes_accessed=12 * wide * d_model + 10 * rows * wide, transcendentals=0),
        )(*kept)

        y_loc = (own[0] + got[0].astype(F32)).astype(BF16)
        du_loc = (own[1] + got[1].astype(F32)).astype(BF16)
        return y_loc, du_loc, dwg, dwu, dwd, dwr.T

    return jax.shard_map(device_step, mesh=mesh, in_specs=in_specs, out_specs=out_specs, check_vma=False)
```
